128 devices in a mesh: row: 8 (over x_lo, z), col: 16 (over y, x_hi, core).
Axes of the slice: x: 4 (x_hi: 2, x_lo: 2; x = x_hi * 2 + x_lo), y: 4, z: 4, core: 2. Of those that a mesh axis runs over, the one named last changes fastest.
Arguments:
- lensed_picture_vectors: bfloat16 [24576, 512], P(('row', 'col')), may hold values from -6 to 6
- theta_feature_vectors: bfloat16 [24576, 512], P(('row', 'col')), may hold values from -6 to 6
- prior_domain_label: int32 [24576], P(('row', 'col')), may hold values from 0 to 63, as said below
- matched_theta_index: int32 [24576], P(('row', 'col')), may hold values from 0 to 24575, each once
- affinity_gain: float32 [1], replicated, may hold values from 5 to 15
- affinity_shift: float32 [1], replicated, may hold values from -4 to -1
Outputs:
- loss: float32 [1], replicated
- grad_data: float32 [24576, 512], P(('row', 'col'))
- grad_param: float32 [24576, 512], P(('row', 'col'))
The draws below stay inside these ranges and needn't reach their ends.
Inputs may be any that keep to these rules, and one draw needn't show every extreme that they name: `matched_theta_index`: a permutation of the pair indices. `prior_domain_label`: region 0 is shared by a share of the pairs that differs between blocks of 192 pairs.
All inputs are finite; a program needn't handle non-finite values.
Results may differ from the reference program's by a relative error of at most 0.00086.
Values may be sent and summed in bfloat16 or wider, within the bound.
A program may use at most 64 MiB of HBM per device.

```python
import math
import jax
import jax.numpy as jnp
from jax import lax

E = 512
ROW_DEV = 192
REGIONS = 64
TOKENS = 24576
N_ROW = 8
N_COL = 16


def shared_part(key, salt):
    groups = TOKENS // ROW_DEV
    direction = jax.random.normal(jax.random.fold_in(key, 101), (E,), jnp.float32)
    key_sign, key_strength = jax.random.split(jax.random.fold_in(key, salt), 2)
    polarity = jnp.where(jax.random.bernoulli(key_sign, 0.5, (TOKENS, 1)), 1.0, -1.0).astype(jnp.float32)
    strength = jax.random.uniform(key_strength, (groups, 1), jnp.float32, 0.0, 2.5)
    strength = jnp.repeat(strength, ROW_DEV, axis=0)
    return strength * polarity * direction[None, :]


def draw_lensed_picture_vectors(key, part):
    key_noise = jax.random.fold_in(key, 211)
    noise = jax.random.normal(key_noise, (TOKENS, E), jnp.float32)
    values = noise + shared_part(key, 307)
    return jnp.clip(values, -6.0, 6.0).astype(jnp.bfloat16)


def draw_theta_feature_vectors(key, part):
    key_noise = jax.random.fold_in(key, 223)
    noise = jax.random.normal(key_noise, (TOKENS, E), jnp.float32)
    values = noise + shared_part(key, 311)
    return jnp.clip(values, -6.0, 6.0).astype(jnp.bfloat16)


def draw_prior_domain_label(key, part):
    groups = TOKENS // ROW_DEV
    key_base, key_spread, key_offset, key_share, key_common, key_factor = jax.random.split(jax.random.fold_in(key, 17), 6)
    common_base = jax.random.randint(key_common, (), 0, REGIONS - 1)
    shared_flag = jax.random.randint(key_share, (groups, 1), 0, 2) == 1
    own_base = jax.random.randint(key_base, (groups, 1), 0, REGIONS - 1)
    base = jnp.where(shared_flag, common_base, own_base)
    spread = jnp.left_shift(jnp.int32(1), jax.random.randint(key_spread, (groups, 1), 0, 7))
    spread = jnp.where(shared_flag, jnp.int32(1), spread)
    shift_amount = jax.random.randint(key_offset, (groups, ROW_DEV), 0, 1 << 30) % spread
    scattered = 1 + (base + shift_amount) % (REGIONS - 1)
    group_index = jnp.arange(groups, dtype=jnp.int32)[:, None]
    row_place = group_index // N_COL
    col_place = group_index % N_COL
    base_count = ROW_DEV * 9 * (row_place + col_place) // (10 * (N_ROW + N_COL - 2))
    factor = jax.random.randint(key_factor, (groups, 1), 5, 11)
    common_count = (base_count * factor + 9) // 10
    position = jnp.arange(ROW_DEV, dtype=jnp.int32)[None, :]
    labels = jnp.where(position < common_count, 0, scattered).reshape(TOKENS)
    labels = labels.at[TOKENS - 1].set(REGIONS - 1)
    return labels.astype(jnp.int32)


def setup_inputs(seed: int = 0) -> dict:
    keys = jax.random.split(jax.random.key(seed), 7)
    lensed_picture_vectors = draw_lensed_picture_vectors(jax.random.fold_in(keys[6], 71), 0)
    theta_feature_vectors = draw_theta_feature_vectors(jax.random.fold_in(keys[6], 71), 0)
    prior_domain_label = draw_prior_domain_label(jax.random.fold_in(keys[6], 71), 0)
    matched_theta_index = jax.random.permutation(keys[3], TOKENS).astype(jnp.int32)
    affinity_gain = jnp.clip(jax.random.uniform(keys[4], (1,), jnp.float32, 5.0, 15.0), 5.0, 15.0)
    affinity_shift = jnp.clip(jax.random.uniform(keys[5], (1,), jnp.float32, -4.0, -1.0), -4.0, -1.0)
    return dict(lensed_picture_vectors=lensed_picture_vectors, theta_feature_vectors=theta_feature_vectors, prior_domain_label=prior_domain_label, matched_theta_index=matched_theta_index, affinity_gain=affinity_gain, affinity_shift=affinity_shift)


def normalize(embed):
    full = embed.astype(jnp.float32)
    scale = lax.rsqrt(lax.optimization_barrier(jnp.mean(full * full, axis=-1, keepdims=True)) + 1e-06)
    full = full * scale
    return (full, scale, full.astype(jnp.bfloat16))

def backward_norm(dnorm, full, scale):
    return scale * (dnorm - full * lax.optimization_barrier(jnp.mean(dnorm * full, axis=-1, keepdims=True)))

def reference(lensed_picture_vectors, theta_feature_vectors, prior_domain_label, matched_theta_index, affinity_gain, affinity_shift):
    data_full, data_scale, data_norm = normalize(lensed_picture_vectors)
    param_full, param_scale, param_norm = normalize(theta_feature_vectors)
    hidden_size = lensed_picture_vectors.shape[1]
    sharpness_coefficient = affinity_gain[0] / hidden_size
    block = math.gcd(512, TOKENS)
    column_entries = jnp.arange(TOKENS, dtype=jnp.int32)

    def step(carry, index):
        param_acc, loss_acc = carry
        start = (index * block).astype(jnp.int32)
        source_count = lax.dynamic_slice_in_dim(data_norm, start, block, 0)
        source_region = lax.dynamic_slice_in_dim(prior_domain_label, start, block, 0)
        source_subset = lax.dynamic_slice_in_dim(matched_theta_index, start, block, 0)
        similarity_value = jnp.dot(source_count, param_norm.T, preferred_element_type=jnp.float32)
        pair_affinity = sharpness_coefficient * similarity_value + affinity_shift[0]
        positive = source_subset[:, None] == column_entries[None, :]
        retain_mask = positive | (source_region[:, None] != prior_domain_label[None, :])
        polarity_value = jnp.where(positive, 1.0, -1.0).astype(jnp.float32)
        partial_loss = jnp.sum(jnp.where(retain_mask, -jax.nn.log_sigmoid(polarity_value * pair_affinity), 0.0))
        pairwise_slope = (jnp.where(retain_mask, -polarity_value * jax.nn.sigmoid(-polarity_value * pair_affinity), 0.0) * sharpness_coefficient).astype(jnp.bfloat16)
        image_embed_gradient = jnp.dot(pairwise_slope, param_norm, preferred_element_type=jnp.float32)
        param_d = jnp.dot(pairwise_slope.T, source_count, preferred_element_type=jnp.float32)
        return ((param_acc + param_d, loss_acc + partial_loss), image_embed_gradient)
    init = (jnp.zeros((TOKENS, hidden_size), jnp.float32), jnp.zeros((), jnp.float32))
    (param_dnorm, total), data_blocks = lax.scan(step, init, jnp.arange(TOKENS // block, dtype=jnp.int32))
    data_dnorm = data_blocks.reshape(TOKENS, hidden_size)
    loss = (total / (TOKENS * TOKENS)).reshape(1).astype(jnp.float32)
    return (loss, backward_norm(data_dnorm, data_full, data_scale), backward_norm(param_dnorm, param_full, param_scale))
```

```python
import functools

import jax
import jax.numpy as jnp
from jax import lax
from jax.sharding import Mesh
from jax.sharding import PartitionSpec as P

COL = ("col_0", "col_1", "col_2")
ROW = ("row_0", "row_1")
ROW_COL = ("row_0", "row_1", "col_0", "col_1", "col_2")


def copy_for_each(x, axis):
    copies = jnp.broadcast_to(x, (lax.axis_size(axis), *x.shape))
    return lax.all_to_all(copies, axis, split_axis=0, concat_axis=0, tiled=True)


def in_order(pieces, dim):
    dims = list(pieces.shape[1:])
    dims[dim] *= pieces.shape[0]
    return jnp.moveaxis(pieces, 0, dim).reshape(dims)


def gather_directly(x, axis, dim):
    pieces = copy_for_each(x, axis)
    return in_order(pieces, dim)


def cut_along(x, dim, devices):
    dims = x.shape
    pieces = x.reshape(*dims[:dim], devices, dims[dim] // devices, *dims[dim + 1 :])
    return jnp.moveaxis(pieces, dim, 0)


def sum_at_owner(x, axis, dim):
    devices = lax.axis_size(axis)
    pieces = lax.all_to_all(cut_along(x, dim, devices), axis, 0, 0, tiled=True)
    return jnp.sum(pieces, axis=0)


def over_axes(x, axes):
    return lax.psum(x, axes)


def normalize(embed):
    full = embed.astype(jnp.float32)
    scale = lax.rsqrt(jnp.mean(full * full, axis=-1, keepdims=True) + 1e-06)
    full = full * scale
    return (full, scale, full.astype(jnp.bfloat16))


def backward_norm(dnorm, full, scale):
    return scale * (dnorm - full * jnp.mean(dnorm * full, axis=-1, keepdims=True))


def tile_terms(
    source_count,
    source_region,
    source_subset,
    target_count,
    target_region,
    target_overall,
    sharpness_coefficient,
    shift_amount,
):
    similarity_value = jnp.dot(source_count, target_count.T, preferred_element_type=jnp.float32)
    pair_affinity = sharpness_coefficient * similarity_value + shift_amount
    positive = source_subset[:, None] == target_overall[None, :]
    retain_mask = positive | (source_region[:, None] != target_region[None, :])
    polarity_value = jnp.where(positive, 1.0, -1.0).astype(jnp.float32)
    partial_loss = jnp.sum(
        jnp.where(retain_mask, -jax.nn.log_sigmoid(polarity_value * pair_affinity), 0.0)
    )
    pairwise_slope = (
        jnp.where(
            retain_mask, -polarity_value * jax.nn.sigmoid(-polarity_value * pair_affinity), 0.0
        )
        * sharpness_coefficient
    ).astype(jnp.bfloat16)
    image_embed_gradient = jnp.dot(pairwise_slope, target_count, preferred_element_type=jnp.float32)
    param_d = lax.dot_general(
        pairwise_slope, source_count, (((0,), (0,)), ((), ())), preferred_element_type=jnp.float32
    )
    return (partial_loss, image_embed_gradient, param_d)


def on_device(
    lensed_picture_vectors,
    theta_feature_vectors,
    prior_domain_label,
    matched_theta_index,
    affinity_gain,
    affinity_shift,
):
    shard = lensed_picture_vectors.shape[0]
    hidden_size = lensed_picture_vectors.shape[1]
    col_count = lax.axis_size(COL)
    row_count = lax.axis_size(ROW)
    col_index = lax.axis_index(COL)
    sharpness_coefficient = affinity_gain[0] / hidden_size
    shift_amount = affinity_shift[0]
    data_full, data_scale, data_norm = normalize(lensed_picture_vectors)
    param_full, param_scale, param_norm = normalize(theta_feature_vectors)
    col_total = shard * row_count
    target_count, target_region = (
        gather_directly(param_norm, ROW, 0),
        gather_directly(prior_domain_label, ROW, 0),
    )
    place = jnp.arange(col_total, dtype=jnp.int32)
    target_overall = place // shard * (shard * col_count) + col_index * shard + place % shard
    source_count = lax.all_gather(data_norm, COL, axis=0, tiled=True)
    packed = gather_directly(matched_theta_index * 64 + prior_domain_label, COL, 0)
    source_region = packed & 63
    source_subset = packed >> 6
    partial_loss, image_embed_gradient, param_d = tile_terms(
        source_count,
        source_region,
        source_subset,
        target_count,
        target_region,
        target_overall,
        sharpness_coefficient,
        shift_amount,
    )
    data_dnorm = lax.psum_scatter(image_embed_gradient, COL, scatter_dimension=0, tiled=True)
    param_dnorm = sum_at_owner(param_d, ROW, 0)
    total = over_axes(partial_loss, ROW_COL)
    pair_total = shard * row_count * col_count
    loss = (total / (pair_total * pair_total)).reshape(1)
    grad_data = backward_norm(data_dnorm, data_full, data_scale)
    grad_param = backward_norm(param_dnorm, param_full, param_scale)
    return (loss, grad_data, grad_param)


def solution(mesh):
    torus = Mesh(mesh.devices.reshape(2, 4, 4, 2, 2), ("row_0", "row_1", "col_0", "col_1", "col_2"))
    in_specs = (P(ROW_COL, None), P(ROW_COL, None), P(ROW_COL), P(ROW_COL), P(), P())
    out_specs = (P(), P(ROW_COL, None), P(ROW_COL, None))
    return jax.shard_map(
        on_device, mesh=torus, in_specs=in_specs, out_specs=out_specs, check_vma=False
    )
```

```python
import jax
import jax.numpy as jnp
from jax import lax
from jax.experimental import pallas as pl
from jax.experimental.pallas import tpu as pltpu
from jax.sharding import PartitionSpec as P

f32 = jnp.float32
bf16 = jnp.bfloat16
i32 = jnp.int32
LOG2E = 1.4426950408889634
LN2 = 0.6931471805599453
MASKED = -1e5
NT = (((1,), (1,)), ((), ()))
NN = (((1,), (0,)), ((), ()))
TN = (((0,), (0,)), ((), ()))
MESH = pl.DeviceIdType.MESH
B = 192
E = 512
V = 4 * B
XU = [(0, 0), (0, 1), (3, 0), (1, 0), (3, 1), (1, 1), (2, 0), (2, 1)]
PZ = [3, 1, 0, 2]
N_GATHER = 22
N_SEM = 2 * N_GATHER + 8 + 14 + 7


def xs(ry, rx, rc=0):
    return 2 * XU.index((ry, rx)) + rc


def ps(rz, rx):
    return 2 * PZ.index(rz) + rx


def rows(slot):
    return pl.ds(slot * B, B)


def pair_terms(s, row_region, row_match, col_region, col_index, gain, gain2, shift2):
    t = s * gain2 + shift2
    positive = row_match == col_index
    t = jnp.where(positive, -t, jnp.where(row_region != col_region, t, MASKED))
    soft = jnp.log2(1.0 + jnp.exp2(t))
    slope = jnp.exp2(t - soft) * jnp.where(positive, -gain, gain)
    return slope.astype(bf16), soft


def fold(x):
    return jnp.sum(x.reshape(x.shape[0] // 8, 8, 128), axis=0)


def kernel(
    gain_ref, shift_ref, x_ref, p_ref, lab_ref,
    loss_ref, gx_ref, gp_ref,
    xb, pb, lx, lp, rr, rm, cr, cj, dx, dp, rc, ry, rz, acc, lsend, lrecv, send_sem, recv_sem,
):
    r, c = lax.axis_index("row"), lax.axis_index("col")
    xl, z = r // 4, r % 4
    y, xh, core = c // 4, (c // 2) % 2, c % 2
    low = c % 4
    cp = (r, c + 1 - 2 * core)
    dxp = ((1 - xl) * 4 + z, c)
    pxp = ((1 - xl) * 4 + z, y * 4 + (1 - xh) * 2 + core)
    yu, yd = (r, ((y + 1) % 4) * 4 + low), (r, ((y + 3) % 4) * 4 + low)
    zu, zd = (xl * 4 + (z + 1) % 4, c), (xl * 4 + (z + 3) % 4, c)

    count = [0]
    pending = []

    def send(src, dst, device):
        k = count[0]
        count[0] += 1
        copy = pltpu.make_async_remote_copy(
            src_ref=src, dst_ref=dst, send_sem=send_sem.at[k], recv_sem=recv_sem.at[k],
            device_id=device, device_id_type=MESH,
        )
        copy.start()
        pending.append(copy)
        return copy

    def normalize(ref):
        full = ref[...].astype(f32)
        scale = lax.rsqrt(jnp.mean(full * full, axis=-1, keepdims=True) + 1e-06)
        return full * scale, scale

    barrier = pltpu.get_barrier_semaphore()
    for peer in (cp, dxp, pxp, yu, yd, zu, zd):
        pl.semaphore_signal(barrier, inc=1, device_id=peer, device_id_type=MESH)
    own_x, own_p = xs(0, 0), ps(0, 0)
    xb[rows(own_x), :] = normalize(x_ref)[0].astype(bf16)
    pb[rows(own_p), :] = normalize(p_ref)[0].astype(bf16)
    lx[own_x] = lab_ref[0, :, 0:256]
    lp[own_p] = lab_ref[0]
    pl.semaphore_wait(barrier, 7)

    got = {}

    def send_x(src, dst, device):
        label = lab_ref.at[0, :, pl.ds(0, 256)] if src == own_x else lx.at[src]
        got["x", dst] = (send(label, lx.at[dst], device), send(xb.at[rows(src)], xb.at[rows(dst)], device))

    def send_p(src, dst, device):
        label = lab_ref.at[0] if src == own_p else lp.at[src]
        got["p", dst] = (send(label, lp.at[dst], device), send(pb.at[rows(src)], pb.at[rows(dst)], device))

    def wait(kind, slot):
        for copy in got[kind, slot]:
            copy.wait_recv()

    def row_info(slot):
        t = jnp.transpose(jnp.broadcast_to(lx[slot], (128, 256)))[0:B]
        rr[rows(slot), :] = t & 63
        rm[rows(slot), :] = t >> 6

    def col_info(rz_):
        first, second = lp[ps(rz_, 0)], lp[ps(rz_, 1)]
        zz = (z + rz_) % 4
        base0 = ((xl * 4 + zz) * 16 + y * 4 + xh * 2 + core) * B
        base1 = (((1 - xl) * 4 + zz) * 16 + y * 4 + (1 - xh) * 2 + core) * B
        lane = lax.broadcasted_iota(i32, (1, 128), 1)
        off = ps(rz_, 0) * B
        parts = (first[:, 0:128], first[:, 128:256] + second[:, 256:384], second[:, 384:512])
        for k in range(3):
            at = lane + k * 128
            cr[:, off + k * 128 : off + (k + 1) * 128] = parts[k] & 63
            cj[:, off + k * 128 : off + (k + 1) * 128] = jnp.where(at < B, base0 + at, base1 + at - B)

    send_x(own_x, xs(0, 1), dxp)
    send_p(own_p, ps(0, 1), pxp)
    send_x(own_x, xs(3, 0), yu)
    send_x(own_x, xs(1, 0), yd)
    send_p(own_p, ps(3, 0), zu)
    send_p(own_p, ps(1, 0), zd)
    send_x(own_x, xs(0, 0, 1), cp)

    dx[...] = jnp.zeros_like(dx)
    dp[...] = jnp.zeros_like(dp)
    acc[...] = jnp.zeros_like(acc)
    row_info(own_x)
    gain = gain_ref[0] / E
    gain2 = gain * LOG2E
    shift2 = shift_ref[0] * LOG2E

    def tile(v, c0, width):
        r0 = pl.multiple_of(v * V, V)
        x = xb[pl.ds(r0, V), :]
        p = pb[pl.ds(c0, width), :]
        s = lax.dot_general(x, p, NT, preferred_element_type=f32)
        region, match = rr[pl.ds(r0, V), :], rm[pl.ds(r0, V), :]
        slopes, total = [], None
        for k in range(width // 128):
            cs = pl.ds(c0 + k * 128, 128)
            slope, soft = pair_terms(
                s[:, k * 128 : (k + 1) * 128], region, match, cr[:, cs], cj[:, cs], gain, gain2, shift2
            )
            slopes.append(slope)
            soft = fold(soft)
            total = soft if total is None else total + soft
        acc[...] += total
        g = jnp.concatenate(slopes, axis=1)
        dx[pl.ds(r0, V), :] += lax.dot_general(g, p, NN, preferred_element_type=f32)
        dp[pl.ds(c0, width), :] += lax.dot_general(g, x, TN, preferred_element_type=f32)

    def run(v0, n, c0, width):
        def body(i, _):
            tile(v0 + i, c0, width)
            return 0

        lax.fori_loop(0, n, body, 0)

    wait("x", xs(0, 1))
    send_x(xs(0, 1), xs(3, 1), yu)
    send_x(xs(0, 1), xs(1, 1), yd)
    send_x(xs(0, 1), xs(0, 1, 1), cp)
    wait("p", ps(0, 1))
    send_p(ps(0, 1), ps(3, 1), zu)
    send_p(ps(0, 1), ps(1, 1), zd)
    wait("x", xs(3, 0))
    send_x(xs(3, 0), xs(2, 0), yu)
    send_x(xs(3, 0), xs(3, 0, 1), cp)
    wait("x", xs(1, 0))
    send_x(xs(1, 0), xs(1, 0, 1), cp)
    wait("p", ps(3, 0))
    send_p(ps(3, 0), ps(2, 0), zu)
    wait("p", ps(1, 0))
    col_info(0)
    for u in ((0, 1), (3, 0), (1, 0)):
        row_info(xs(*u))
    for u in ((0, 0), (0, 1), (3, 0), (1, 0)):
        wait("x", xs(*u, 1))
        row_info(xs(*u, 1))
    run(0, 2, 2 * V // 2, V // 2)

    wait("x", xs(1, 1))
    send_x(xs(1, 1), xs(2, 1), yd)
    send_x(xs(1, 1), xs(1, 1, 1), cp)
    wait("p", ps(1, 1))
    send_p(ps(1, 1), ps(2, 1), zd)
    wait("x", xs(3, 1))
    send_x(xs(3, 1), xs(3, 1, 1), cp)
    wait("p", ps(3, 1))
    col_info(3)
    col_info(1)
    run(0, 2, 0, V)

    for u in ((2, 0), (2, 1)):
        wait("x", xs(*u))
        send_x(xs(*u), xs(*u, 1), cp)
    wait("p", ps(2, 0))
    wait("p", ps(2, 1))
    col_info(2)
    for u in ((3, 1), (1, 1)):
        row_info(xs(*u))
        wait("x", xs(*u, 1))
        row_info(xs(*u, 1))
    for u in ((2, 0), (2, 1)):
        row_info(xs(*u))
        wait("x", xs(*u, 1))
        row_info(xs(*u, 1))
    tile(3, V, V)
    tile(3, 0, V)

    half = {}

    def to_core(u):
        k = XU.index(u)
        half[u] = send(dx.at[rows(xs(*u, 1))], rc.at[k], cp)

    def add_core(u):
        half[u].wait_recv()
        dx[rows(xs(*u)), :] += rc[XU.index(u)]

    def send_dx(u, k, device):
        return send(dx.at[rows(xs(*u))], ry.at[k], device)

    def send_dp(u, k, device):
        return send(dp.at[rows(ps(*u))], rz.at[k], device)

    def add_dx(u, k, copy):
        copy.wait_recv()
        dx[rows(xs(*u)), :] += ry[k]

    def add_dp(u, k, copy):
        copy.wait_recv()
        dp[rows(ps(*u)), :] += rz[k]

    to_core((2, 0))
    to_core((2, 1))
    tile(0, 3 * V // 2, V // 2)
    add_core((2, 0))
    xa = send_dx((2, 0), 0, yd)
    add_core((2, 1))
    xb_ = send_dx((2, 1), 1, yu)
    tile(1, 3 * V // 2, V // 2)
    for u in ((0, 0), (0, 1), (3, 0), (1, 0)):
        to_core(u)
    tile(2, V, V)
    pa = send_dp((2, 0), 0, zd)
    pb_ = send_dp((2, 1), 1, zu)
    for u in ((0, 0), (0, 1), (3, 0), (1, 0)):
        add_core(u)
    tile(2, 0, V)
    to_core((3, 1))
    to_core((1, 1))

    lsend[0] = jnp.sum(acc[...], axis=0, keepdims=True)
    y1 = (r, (y + 1 - 2 * (y % 2)) * 4 + low)
    y2 = (r, (3 - y) * 4 + low)
    z1 = (xl * 4 + z + 1 - 2 * (z % 2), c)
    z2 = (xl * 4 + 3 - z, c)
    stages = [cp, dxp, pxp, y1, y2, z1, z2]
    exchange = [None] * 7

    def loss_send(k):
        exchange[k] = send(lsend.at[k], lrecv.at[k], stages[k])

    def loss_add(k):
        exchange[k].wait_recv()
        lsend[k + 1] = lsend[k] + lrecv[k]

    add_core((3, 1))
    xd = send_dx((3, 1), 3, yd)
    pd = send_dp((3, 1), 3, zd)
    add_core((1, 1))
    add_dx((1, 1), 1, xb_)
    xf = send_dx((1, 1), 5, yu)
    loss_send(0)
    add_dx((3, 0), 0, xa)
    xc = send_dx((3, 0), 2, yd)
    xe = send_dx((1, 0), 4, yu)
    loss_add(0)
    loss_send(1)
    add_dp((1, 1), 1, pb_)
    pf = send_dp((1, 1), 5, zu)
    pe = send_dp((1, 0), 4, zu)
    add_dp((3, 0), 0, pa)
    pc = send_dp((3, 0), 2, zd)
    loss_add(1)
    loss_send(2)
    add_dx((0, 1), 3, xd)
    loss_add(2)
    loss_send(3)
    add_dx((0, 1), 5, xf)
    xg = send_dx((0, 1), 6, dxp)
    loss_add(3)
    loss_send(4)
    add_dp((0, 1), 3, pd)
    add_dp((0, 1), 5, pf)
    pg = send_dp((0, 1), 6, pxp)
    loss_add(4)
    loss_send(5)
    add_dx((0, 0), 2, xc)
    add_dx((0, 0), 4, xe)
    loss_add(5)
    loss_send(6)
    add_dp((0, 0), 2, pc)
    add_dp((0, 0), 4, pe)
    loss_add(6)
    n = float(128 * B)
    loss_ref[0] = jnp.sum(lsend[7]) * LN2 / (n * n)

    def finish(ref, dnorm, out):
        full, scale = normalize(ref)
        out[...] = scale * (dnorm - full * jnp.mean(dnorm * full, axis=-1, keepdims=True))

    xg.wait_recv()
    finish(x_ref, dx[rows(own_x), :] + ry[6], gx_ref)
    pg.wait_recv()
    finish(p_ref, dp[rows(own_p), :] + rz[6], gp_ref)
    for copy in pending:
        copy.wait_send()
    assert count[0] == N_SEM


def on_device(lensed, theta, region, match, gain, shift):
    packed = match * 64 + region
    lab = jnp.concatenate([jnp.pad(packed, (0, 64)), jnp.pad(packed, (64, 0))]).reshape(1, 1, 512)
    vmem = pl.BlockSpec(memory_space=pltpu.VMEM)
    smem = pl.BlockSpec(memory_space=pltpu.SMEM)
    return pl.pallas_call(
        kernel,
        out_shape=(
            jax.ShapeDtypeStruct((1,), f32),
            jax.ShapeDtypeStruct((B, E), f32),
            jax.ShapeDtypeStruct((B, E), f32),
        ),
        in_specs=[smem, smem, vmem, vmem, vmem],
        out_specs=(smem, vmem, vmem),
        scratch_shapes=[
            pltpu.VMEM((16 * B, E), bf16),
            pltpu.VMEM((8 * B, E), bf16),
            pltpu.VMEM((16, 1, 256), i32),
            pltpu.VMEM((8, 1, 512), i32),
            pltpu.VMEM((16 * B, 128), i32),
            pltpu.VMEM((16 * B, 128), i32),
            pltpu.VMEM((1, 8 * B), i32),
            pltpu.VMEM((1, 8 * B), i32),
            pltpu.VMEM((16 * B, E), f32),
            pltpu.VMEM((8 * B, E), f32),
            pltpu.VMEM((8, B, E), f32),
            pltpu.VMEM((7, B, E), f32),
            pltpu.VMEM((7, B, E), f32),
            pltpu.VMEM((8, 128), f32),
            pltpu.VMEM((8, 1, 128), f32),
            pltpu.VMEM((7, 1, 128), f32),
            pltpu.SemaphoreType.DMA((N_SEM,)),
            pltpu.SemaphoreType.DMA((N_SEM,)),
        ],
        compiler_params=pltpu.CompilerParams(
            collective_id=0, has_side_effects=True, vmem_limit_bytes=60 << 20
        ),
        name="pairs",
    )(gain, shift, lensed, theta, lab)


def solution(mesh):
    both = ("row", "col")
    in_specs = (P(both, None), P(both, None), P(both), P(both), P(), P())
    out_specs = (P(), P(both, None), P(both, None))
    return jax.shard_map(
        on_device, mesh=mesh, in_specs=in_specs, out_specs=out_specs, check_vma=False
    )
```

```python
import jax
import jax.numpy as jnp
from jax import lax
from jax.experimental import pallas as pl
from jax.experimental.pallas import tpu as pltpu
from jax.sharding import PartitionSpec as P

f32 = jnp.float32
bf16 = jnp.bfloat16
i32 = jnp.int32
LOG2E = 1.4426950408889634
LN2 = 0.6931471805599453
MASKED = -1e5
NT = (((1,), (1,)), ((), ()))
NN = (((1,), (0,)), ((), ()))
TN = (((0,), (0,)), ((), ()))
MESH = pl.DeviceIdType.MESH
B = 192
E = 512
V = 4 * B
H = B // 2
XU = [(0, 0), (0, 1), (3, 0), (1, 0), (3, 1), (1, 1), (2, 0), (2, 1)]
PU = [(2, 0), (2, 1), (3, 1), (1, 1), (0, 0), (0, 1), (3, 0), (1, 0)]
N_SEM = 7 * 3 + 8 * 2 + 7 * 3 + 8 + 2 * 7 * 2 + 10


def xs(ry, rx, rc=0):
    return 2 * XU.index((ry, rx)) + rc


def ps(rz, rx):
    return PU.index((rz, rx))


def part(slot, h):
    return pl.ds(slot * B + h * H, H)


def rows(slot):
    return pl.ds(slot * B, B)


def pair_terms(s, row_region, row_match, col_region, col_index, gain, gain2, shift2):
    t = s * gain2 + shift2
    positive = row_match == col_index
    t = jnp.where(positive, -t, jnp.where(row_region != col_region, t, MASKED))
    soft = jnp.log2(1.0 + jnp.exp2(t))
    slope = jnp.exp2(t - soft) * jnp.where(positive, -gain, gain)
    return slope.astype(bf16), soft


def fold(x):
    return jnp.sum(x.reshape(x.shape[0] // 8, 8, 128), axis=0)


def normalize(ref):
    full = ref[...].astype(f32)
    scale = lax.rsqrt(jnp.mean(full * full, axis=-1, keepdims=True) + 1e-06)
    return full * scale, scale


def kernel(
    gain_ref, shift_ref, *hbm_and_rest,
):
    hbm, rest = hbm_and_rest[:4], hbm_and_rest[4:]
    pair_kernel(gain_ref, shift_ref, hbm, *rest)


def pair_kernel(
    gain_ref, shift_ref, hbm,
    loss_ref, sx_ref, sp_ref,
    x_ref, p_ref, region_ref, match_ref, in_sem,
    xb, pb, lab_ref, lx, lp, rr, rm, cr, cj, dx, dp, rc, ry, rz, acc, lsend, lrecv, send_sem, recv_sem,
):
    r, c = lax.axis_index("row"), lax.axis_index("col")
    xl, z = r // 4, r % 4
    y, xh, core = c // 4, (c // 2) % 2, c % 2
    low = c % 4
    cp = (r, c + 1 - 2 * core)
    dxp = ((1 - xl) * 4 + z, c)
    pxp = ((1 - xl) * 4 + z, y * 4 + (1 - xh) * 2 + core)
    xo = (r, y * 4 + (1 - xh) * 2 + core)
    yu, yo, yd = ((r, ((y + k) % 4) * 4 + low) for k in (1, 2, 3))
    zu, zo, zd = ((xl * 4 + (z + k) % 4, c) for k in (1, 2, 3))

    count = [0]
    pending = []

    def send(src, dst, device):
        k = count[0]
        count[0] += 1
        copy = pltpu.make_async_remote_copy(
            src_ref=src, dst_ref=dst, send_sem=send_sem.at[k], recv_sem=recv_sem.at[k],
            device_id=device, device_id_type=MESH,
        )
        copy.start()
        pending.append(copy)
        return copy

    loads = [
        pltpu.make_async_copy(src, dst, in_sem.at[k])
        for k, (src, dst) in enumerate(zip(hbm, (x_ref, p_ref, region_ref, match_ref)))
    ]
    for load in loads:
        load.start()
    barrier = pltpu.get_barrier_semaphore()
    for peer in (cp, dxp, pxp, xo, yu, yo, yd, zu, zo, zd):
        pl.semaphore_signal(barrier, inc=1, device_id=peer, device_id_type=MESH)
    own_x, own_p = xs(0, 0), ps(0, 0)
    acc[...] = jnp.zeros_like(acc)
    for load in loads:
        load.wait()
    xb[rows(own_x), :] = normalize(x_ref)[0].astype(bf16)
    pb[rows(own_p), :] = normalize(p_ref)[0].astype(bf16)
    packed = match_ref[...] * 64 + region_ref[...]
    wide = jnp.concatenate([packed, jnp.zeros((1, 64), i32)], axis=1)
    lab_ref[0] = jnp.concatenate([wide, pltpu.roll(wide, 64, 1)], axis=1)
    lx[own_x] = wide
    lp[own_p] = lab_ref[0]
    pl.semaphore_wait(barrier, 10)

    got = {}

    def send_x(src, dst, device, h):
        if h == 0:
            label = lab_ref.at[0, :, pl.ds(0, 256)] if src == own_x else lx.at[src]
            got["x", dst, "label"] = send(label, lx.at[dst], device)
        got["x", dst, h] = send(xb.at[part(src, h)], xb.at[part(dst, h)], device)

    def send_p(src, dst, device, h):
        if h == 0:
            label = lab_ref.at[0] if src == own_p else lp.at[src]
            got["p", dst, "label"] = send(label, lp.at[dst], device)
        got["p", dst, h] = send(pb.at[part(src, h)], pb.at[part(dst, h)], device)

    def wait(kind, slot, h):
        if h == 0:
            got[kind, slot, "label"].wait_recv()
        got[kind, slot, h].wait_recv()

    def send_core(u):
        src, dst = xs(*u), xs(*u, 1)
        label = lab_ref.at[0, :, pl.ds(0, 256)] if src == own_x else lx.at[src]
        got["core", u] = (send(label, lx.at[dst], cp), send(xb.at[rows(src)], xb.at[rows(dst)], cp))

    def row_info(slot):
        t = jnp.transpose(jnp.broadcast_to(lx[slot], (128, 256)))[0:B]
        rr[rows(slot), :] = t & 63
        rm[rows(slot), :] = t >> 6

    def rows_ready(u):
        row_info(xs(*u))
        for copy in got["core", u]:
            copy.wait_recv()
        row_info(xs(*u, 1))

    def base(rz_, rx):
        zz = (z + rz_) % 4
        if rx == 0:
            return ((xl * 4 + zz) * 16 + y * 4 + xh * 2 + core) * B
        return (((1 - xl) * 4 + zz) * 16 + y * 4 + (1 - xh) * 2 + core) * B

    def col_info(k0):
        first, second = lp[k0], lp[k0 + 1]
        base0, base1 = base(*PU[k0]), base(*PU[k0 + 1])
        lane = lax.broadcasted_iota(i32, (1, 128), 1)
        parts = (first[:, 0:128], first[:, 128:256] + second[:, 256:384], second[:, 384:512])
        for k in range(3):
            at = lane + k * 128
            cs = pl.ds(k0 * B + k * 128, 128)
            cr[:, cs] = parts[k] & 63
            cj[:, cs] = jnp.where(at < B, base0 + at, base1 + at - B)

    for h in (0, 1):
        send_x(own_x, xs(0, 1), dxp, h)
        send_p(own_p, ps(0, 1), pxp, h)
        send_x(own_x, xs(3, 0), yu, h)
        send_x(own_x, xs(1, 0), yd, h)
        send_p(own_p, ps(3, 0), zu, h)
        send_p(own_p, ps(1, 0), zd, h)
    send_core((0, 0))

    gain = gain_ref[...] / E
    gain2 = gain * LOG2E
    shift2 = shift_ref[...] * LOG2E

    def tile(v, c0, width, new_row=False, new_col=False, add_col=None):
        r0 = v * V
        x = xb[pl.ds(r0, V), :]
        p = pb[pl.ds(c0, width), :]
        s = lax.dot_general(x, p, NT, preferred_element_type=f32)
        region, match = rr[pl.ds(r0, V), :], rm[pl.ds(r0, V), :]
        slopes, total = [], None
        for k in range(width // 128):
            cs = pl.ds(c0 + k * 128, 128)
            slope, soft = pair_terms(
                s[:, k * 128 : (k + 1) * 128], region, match, cr[:, cs], cj[:, cs], gain, gain2, shift2
            )
            slopes.append(slope)
            soft = fold(soft)
            total = soft if total is None else total + soft
        acc[...] += total
        g = jnp.concatenate(slopes, axis=1)
        d_row = lax.dot_general(g, p, NN, preferred_element_type=f32)
        dx[pl.ds(r0, V), :] = d_row if new_row else dx[pl.ds(r0, V), :] + d_row
        cut = width if new_col else 0 if add_col is None else add_col - c0
        for lo, hi, new in ((0, cut, True), (cut, width, False)):
            if lo < hi:
                d_col = lax.dot_general(g[:, lo:hi], x, TN, preferred_element_type=f32)
                at = pl.ds(c0 + lo, hi - lo)
                dp[at, :] = d_col if new else dp[at, :] + d_col

    C1, END = 512, 2 * V

    def cols(v, lo, hi, **new):
        tile(v, lo, hi - lo, **new)

    for h in (0, 1):
        wait("x", xs(3, 0), h)
        send_x(xs(3, 0), xs(2, 0), yu, h)
        wait("p", ps(3, 0), h)
        send_p(ps(3, 0), ps(2, 0), zu, h)
        wait("x", xs(0, 1), h)
        send_x(xs(0, 1), xs(1, 1), yd, h)
        wait("p", ps(0, 1), h)
        send_p(ps(0, 1), ps(1, 1), zd, h)
    for h in (0, 1):
        send_x(xs(0, 1), xs(3, 1), yu, h)
        send_p(ps(0, 1), ps(3, 1), zu, h)
    send_core((0, 1))
    send_core((3, 0))
    for h in (0, 1):
        wait("x", xs(1, 0), h)
    send_core((1, 0))
    for h in (0, 1):
        wait("p", ps(1, 0), h)
    col_info(4)
    col_info(6)
    rows_ready((0, 0))
    rows_ready((0, 1))
    cols(0, V, V + 384, new_row=True, new_col=True)
    for h in (0, 1):
        wait("x", xs(1, 1), h)
        send_x(xs(1, 1), xs(2, 1), yd, h)
        wait("p", ps(1, 1), h)
        send_p(ps(1, 1), ps(2, 1), zd, h)
        if h == 0:
            cols(0, V + 384, END, new_col=True)
    send_core((1, 1))
    for h in (0, 1):
        wait("x", xs(2, 0), h)
    send_core((2, 0))
    rows_ready((3, 0))
    rows_ready((1, 0))
    cols(1, V, END, new_row=True)
    rows_ready((2, 0))

    for h in (0, 1):
        wait("x", xs(2, 1), h)
    send_core((2, 1))
    for h in (0, 1):
        wait("x", xs(3, 1), h)
    send_core((3, 1))
    for u in ((2, 0), (2, 1), (3, 1)):
        for h in (0, 1):
            wait("p", ps(*u), h)
    col_info(0)
    col_info(2)
    rows_ready((2, 1))
    cols(3, 0, END, new_row=True, add_col=V)

    half = {}
    back = {}

    def to_core(u):
        half[u] = send(dx.at[rows(xs(*u, 1))], rc.at[XU.index(u)], cp)

    def add_core(u):
        half[u].wait_recv()
        dx[rows(xs(*u)), :] += rc[XU.index(u)]

    def send_dx(u, k, device, h):
        back["x", k, h] = send(dx.at[part(xs(*u), h)], ry.at[k, pl.ds(h * H, H)], device)

    def send_dp(u, k, device, h):
        back["p", k, h] = send(dp.at[part(ps(*u), h)], rz.at[k, pl.ds(h * H, H)], device)

    def add_dx(u, k, h):
        back["x", k, h].wait_recv()
        dx[part(xs(*u), h), :] += ry[k, pl.ds(h * H, H)]

    def add_dp(u, k, h):
        back["p", k, h].wait_recv()
        dp[part(ps(*u), h), :] += rz[k, pl.ds(h * H, H)]

    ring = {}

    def loss_send(k, peers):
        for n, peer in enumerate(peers):
            ring[k, n] = send(lsend.at[k], lrecv.at[3 * k + n], peer)

    def loss_add(k, n):
        for m in range(n):
            ring[k, m].wait_recv()
        if n == 1:
            lsend[k + 1] = lsend[k] + lrecv[3 * k]
        else:
            lsend[k + 1] = (lsend[k] + lrecv[3 * k]) + (lrecv[3 * k + 1] + lrecv[3 * k + 2])

    to_core((2, 0))
    to_core((2, 1))
    cols(0, 0, C1)
    add_core((2, 0))
    add_core((2, 1))
    for h in (0, 1):
        send_dx((2, 0), 0, yd, h)
        send_dx((2, 1), 1, yu, h)
    cols(1, 0, C1)
    rows_ready((3, 1))
    rows_ready((1, 1))
    cols(2, 0, C1, new_row=True)
    for h in (0, 1):
        send_dp((2, 0), 0, zd, h)
        send_dp((2, 1), 1, zu, h)
    cols(2, C1, END)
    to_core((1, 1))
    to_core((3, 1))
    send_dp((0, 1), 6, pxp, 1)
    cols(0, C1, V)
    add_core((1, 1))
    add_core((3, 1))
    send_dx((3, 1), 3, dxp, 1)
    send_dx((3, 1), 3, yd, 0)
    add_dx((1, 1), 1, 0)
    send_dx((1, 1), 5, yu, 0)
    cols(1, C1, V)
    lsend[0] = jnp.sum(acc[...], axis=0, keepdims=True)
    loss_send(0, (cp,))
    for u in ((3, 0), (1, 0), (0, 1), (0, 0)):
        to_core(u)
    send_dp((3, 1), 3, pxp, 1)
    send_dp((3, 1), 3, zd, 0)
    add_dx((1, 1), 1, 1)
    send_dx((1, 1), 5, dxp, 1)
    add_dp((1, 1), 1, 0)
    send_dp((1, 1), 5, zu, 0)
    add_dp((3, 0), 0, 0)
    send_dp((3, 0), 2, zd, 0)
    send_dp((1, 0), 4, zu, 0)
    loss_add(0, 1)
    loss_send(1, (yo, yu, yd))
    add_core((3, 0))
    add_dx((3, 0), 0, 0)
    send_dx((3, 0), 2, yd, 0)
    add_core((1, 0))
    send_dx((1, 0), 4, yu, 0)
    add_core((0, 1))
    add_core((0, 0))
    add_dx((3, 0), 0, 1)
    add_dp((1, 1), 1, 1)
    send_dp((1, 1), 5, pxp, 1)
    add_dp((3, 0), 0, 1)
    add_dx((0, 1), 3, 0)
    add_dx((0, 1), 5, 0)
    send_dx((0, 1), 6, dxp, 0)
    add_dx((3, 0), 3, 1)
    send_dx((3, 0), 2, yd, 1)
    loss_add(1, 3)
    loss_send(2, (xo, dxp, pxp))
    send_dx((0, 1), 6, dxp, 1)
    add_dp((3, 0), 3, 1)
    send_dp((3, 0), 2, zd, 1)
    add_dx((1, 0), 5, 1)
    send_dx((1, 0), 4, yu, 1)
    add_dp((0, 1), 3, 0)
    add_dp((0, 1), 5, 0)
    send_dp((0, 1), 6, pxp, 0)
    add_dp((1, 0), 5, 1)
    loss_add(2, 3)
    loss_send(3, (zo, zu, zd))
    send_dp((1, 0), 4, zu, 1)
    add_dx((0, 0), 2, 0)
    add_dx((0, 0), 4, 0)
    add_dp((0, 0), 6, 1)
    add_dx((0, 0), 6, 0)
    add_dp((0, 0), 2, 0)
    add_dp((0, 0), 4, 0)
    add_dx((0, 0), 4, 1)
    add_dx((0, 0), 2, 1)
    add_dx((0, 0), 6, 1)
    sx_ref[...] = dx[rows(own_x), :]
    loss_add(3, 3)
    loss_ref[...] = lsend[4]
    add_dp((0, 0), 2, 1)
    add_dp((0, 0), 6, 0)
    add_dp((0, 0), 4, 1)
    sp_ref[...] = dp[rows(own_p), :]
    for copy in pending:
        copy.wait_send()
    assert count[0] == N_SEM


def finish(x_ref, p_ref, sx_ref, sp_ref, sum_ref, loss_ref, gx_ref, gp_ref):
    for ref, sums, out in ((x_ref, sx_ref, gx_ref), (p_ref, sp_ref, gp_ref)):
        full, scale = normalize(ref)
        dnorm = sums[...]
        out[...] = scale * (dnorm - full * jnp.mean(dnorm * full, axis=-1, keepdims=True))
    n = float(128 * B)
    loss_ref[0] = jnp.sum(sum_ref[...]) * LN2 / (n * n)


def on_device(lensed, theta, region, match, gain, shift):
    vmem = pl.BlockSpec(memory_space=pltpu.VMEM)
    smem = pl.BlockSpec(memory_space=pltpu.SMEM)
    block = jax.ShapeDtypeStruct((B, E), f32)
    total, sum_x, sum_p = pl.pallas_call(
        kernel,
        out_shape=(jax.ShapeDtypeStruct((1, 128), f32), block, block),
        in_specs=[vmem] * 2 + [pl.BlockSpec(memory_space=pltpu.HBM)] * 4,
        out_specs=(vmem,) * 3,
        scratch_shapes=[
            pltpu.VMEM((B, E), bf16),
            pltpu.VMEM((B, E), bf16),
            pltpu.VMEM((1, B), i32),
            pltpu.VMEM((1, B), i32),
            pltpu.SemaphoreType.DMA((4,)),
            pltpu.VMEM((16 * B, E), bf16),
            pltpu.VMEM((8 * B, E), bf16),
            pltpu.VMEM((1, 1, 512), i32),
            pltpu.VMEM((16, 1, 256), i32),
            pltpu.VMEM((8, 1, 512), i32),
            pltpu.VMEM((16 * B, 128), i32),
            pltpu.VMEM((16 * B, 128), i32),
            pltpu.VMEM((1, 8 * B), i32),
            pltpu.VMEM((1, 8 * B), i32),
            pltpu.VMEM((16 * B, E), f32),
            pltpu.VMEM((8 * B, E), f32),
            pltpu.VMEM((8, B, E), f32),
            pltpu.VMEM((7, B, E), f32),
            pltpu.VMEM((7, B, E), f32),
            pltpu.VMEM((8, 128), f32),
            pltpu.VMEM((5, 1, 128), f32),
            pltpu.VMEM((12, 1, 128), f32),
            pltpu.SemaphoreType.DMA((N_SEM,)),
            pltpu.SemaphoreType.DMA((N_SEM,)),
        ],
        compiler_params=pltpu.CompilerParams(
            collective_id=0, has_side_effects=True, vmem_limit_bytes=67043328
        ),
        name="pairs",
    )(gain.reshape(1, 1), shift.reshape(1, 1), lensed, theta, region.reshape(1, B), match.reshape(1, B))
    return pl.pallas_call(
        finish,
        out_shape=(jax.ShapeDtypeStruct((1,), f32), block, block),
        in_specs=[vmem] * 5,
        out_specs=(smem, vmem, vmem),
        compiler_params=pltpu.CompilerParams(vmem_limit_bytes=67043328),
        name="finish",
    )(lensed, theta, sum_x, sum_p, total)


def solution(mesh):
    both = ("row", "col")
    in_specs = (P(both, None), P(both, None), P(both), P(both), P(), P())
    out_specs = (P(), P(both, None), P(both, None))
    return jax.shard_map(
        on_device, mesh=mesh, in_specs=in_specs, out_specs=out_specs, check_vma=False
    )
```

```python
import jax
import jax.numpy as jnp
from jax import lax
from jax.experimental import pallas as pl
from jax.experimental.pallas import tpu as pltpu
from jax.sharding import PartitionSpec as P

f32 = jnp.float32
bf16 = jnp.bfloat16
i32 = jnp.int32
LOG2E = 1.4426950408889634
LN2 = 0.6931471805599453
MASKED = -1e5
NT = (((1,), (1,)), ((), ()))
NN = (((1,), (0,)), ((), ()))
TN = (((0,), (0,)), ((), ()))
MESH = pl.DeviceIdType.MESH
B = 192
E = 512
V = 4 * B
H = B // 2
XU = [(0, 0), (0, 1), (3, 0), (1, 0), (3, 1), (1, 1), (2, 0), (2, 1)]
PU = [(2, 0), (2, 1), (3, 1), (1, 1), (0, 0), (0, 1), (3, 0), (1, 0)]
N_SEM = 7 * 3 + 8 * 2 + 7 * 3 + 8 + 2 * 7 * 2 + 10


def xs(ry, rx, rc=0):
    return 2 * XU.index((ry, rx)) + rc


def ps(rz, rx):
    return PU.index((rz, rx))


def part(slot, h):
    return pl.ds(slot * B + h * H, H)


def rows(slot):
    return pl.ds(slot * B, B)


def pair_terms(s, row_region, row_match, col_region, col_index, gain, gain2, shift2):
    t = s * gain2 + shift2
    positive = row_match == col_index
    t = jnp.where(positive, -t, jnp.where(row_region != col_region, t, MASKED))
    soft = jnp.log2(1.0 + jnp.exp2(t))
    slope = jnp.exp2(t - soft) * jnp.where(positive, -gain, gain)
    return slope.astype(bf16), soft


def fold(x):
    return jnp.sum(x.reshape(x.shape[0] // 8, 8, 128), axis=0)


def normalize(ref):
    full = ref[...].astype(f32)
    scale = lax.rsqrt(jnp.mean(full * full, axis=-1, keepdims=True) + 1e-06)
    return full * scale, scale


def kernel(
    gain_ref, shift_ref, *hbm_and_rest,
):
    hbm, rest = hbm_and_rest[:4], hbm_and_rest[4:]
    pair_kernel(gain_ref, shift_ref, hbm, *rest)


def pair_kernel(
    gain_ref, shift_ref, hbm,
    loss_ref, sx_ref, sp_ref, xo_ref, po_ref,
    x_ref, p_ref, region_ref, match_ref, in_sem,
    xb, pb, lab_ref, lx, lp, rr, rm, cr, cj, dx, dp, rc, ry, rz, acc, lsend, lrecv, send_sem, recv_sem,
):
    r, c = lax.axis_index("row"), lax.axis_index("col")
    xl, z = r // 4, r % 4
    y, xh, core = c // 4, (c // 2) % 2, c % 2
    low = c % 4
    cp = (r, c + 1 - 2 * core)
    dxp = ((1 - xl) * 4 + z, c)
    pxp = ((1 - xl) * 4 + z, y * 4 + (1 - xh) * 2 + core)
    xo = (r, y * 4 + (1 - xh) * 2 + core)
    yu, yo, yd = ((r, ((y + k) % 4) * 4 + low) for k in (1, 2, 3))
    zu, zo, zd = ((xl * 4 + (z + k) % 4, c) for k in (1, 2, 3))

    count = [0]
    pending = []

    def send(src, dst, device):
        k = count[0]
        count[0] += 1
        copy = pltpu.make_async_remote_copy(
            src_ref=src, dst_ref=dst, send_sem=send_sem.at[k], recv_sem=recv_sem.at[k],
            device_id=device, device_id_type=MESH,
        )
        copy.start()
        pending.append(copy)
        return copy

    loads = [
        pltpu.make_async_copy(src, dst, in_sem.at[k])
        for k, (src, dst) in enumerate(zip(hbm, (x_ref, p_ref, region_ref, match_ref)))
    ]
    for load in loads:
        load.start()
    barrier = pltpu.get_barrier_semaphore()
    for peer in (cp, dxp, pxp, xo, yu, yo, yd, zu, zo, zd):
        pl.semaphore_signal(barrier, inc=1, device_id=peer, device_id_type=MESH)
    own_x, own_p = xs(0, 0), ps(0, 0)
    acc[...] = jnp.zeros_like(acc)
    for load in loads:
        load.wait()
    xb[rows(own_x), :] = normalize(x_ref)[0].astype(bf16)
    pb[rows(own_p), :] = normalize(p_ref)[0].astype(bf16)
    xo_ref[...] = x_ref[...]
    po_ref[...] = p_ref[...]
    packed = match_ref[...] * 64 + region_ref[...]
    wide = jnp.concatenate([packed, jnp.zeros((1, 64), i32)], axis=1)
    lab_ref[0] = jnp.concatenate([wide, pltpu.roll(wide, 64, 1)], axis=1)
    lx[own_x] = wide
    lp[own_p] = lab_ref[0]
    pl.semaphore_wait(barrier, 10)

    got = {}

    def send_x(src, dst, device, h):
        if h == 0:
            label = lab_ref.at[0, :, pl.ds(0, 256)] if src == own_x else lx.at[src]
            got["x", dst, "label"] = send(label, lx.at[dst], device)
        got["x", dst, h] = send(xb.at[part(src, h)], xb.at[part(dst, h)], device)

    def send_p(src, dst, device, h):
        if h == 0:
            label = lab_ref.at[0] if src == own_p else lp.at[src]
            got["p", dst, "label"] = send(label, lp.at[dst], device)
        got["p", dst, h] = send(pb.at[part(src, h)], pb.at[part(dst, h)], device)

    def wait(kind, slot, h):
        if h == 0:
            got[kind, slot, "label"].wait_recv()
        got[kind, slot, h].wait_recv()

    def send_core(u):
        src, dst = xs(*u), xs(*u, 1)
        label = lab_ref.at[0, :, pl.ds(0, 256)] if src == own_x else lx.at[src]
        got["core", u] = (send(label, lx.at[dst], cp), send(xb.at[rows(src)], xb.at[rows(dst)], cp))

    def row_info(slot):
        t = jnp.transpose(jnp.broadcast_to(lx[slot], (128, 256)))[0:B]
        rr[rows(slot), :] = t & 63
        rm[rows(slot), :] = t >> 6

    def rows_ready(u):
        row_info(xs(*u))
        for copy in got["core", u]:
            copy.wait_recv()
        row_info(xs(*u, 1))

    def base(rz_, rx):
        zz = (z + rz_) % 4
        if rx == 0:
            return ((xl * 4 + zz) * 16 + y * 4 + xh * 2 + core) * B
        return (((1 - xl) * 4 + zz) * 16 + y * 4 + (1 - xh) * 2 + core) * B

    def col_info(k0):
        first, second = lp[k0], lp[k0 + 1]
        base0, base1 = base(*PU[k0]), base(*PU[k0 + 1])
        lane = lax.broadcasted_iota(i32, (1, 128), 1)
        parts = (first[:, 0:128], first[:, 128:256] + second[:, 256:384], second[:, 384:512])
        for k in range(3):
            at = lane + k * 128
            cs = pl.ds(k0 * B + k * 128, 128)
            cr[:, cs] = parts[k] & 63
            cj[:, cs] = jnp.where(at < B, base0 + at, base1 + at - B)

    for h in (0, 1):
        send_x(own_x, xs(0, 1), dxp, h)
        send_p(own_p, ps(0, 1), pxp, h)
        send_x(own_x, xs(3, 0), yu, h)
        send_x(own_x, xs(1, 0), yd, h)
        send_p(own_p, ps(3, 0), zu, h)
        send_p(own_p, ps(1, 0), zd, h)
    send_core((0, 0))

    gain = gain_ref[...] / E
    gain2 = gain * LOG2E
    shift2 = shift_ref[...] * LOG2E

    def tile(v, c0, width, new_row=False, new_col=False, add_col=None):
        r0 = v * V
        x = xb[pl.ds(r0, V), :]
        p = pb[pl.ds(c0, width), :]
        s = lax.dot_general(x, p, NT, preferred_element_type=f32)
        region, match = rr[pl.ds(r0, V), :], rm[pl.ds(r0, V), :]
        slopes, total = [], None
        for k in range(width // 128):
            cs = pl.ds(c0 + k * 128, 128)
            slope, soft = pair_terms(
                s[:, k * 128 : (k + 1) * 128], region, match, cr[:, cs], cj[:, cs], gain, gain2, shift2
            )
            slopes.append(slope)
            soft = fold(soft)
            total = soft if total is None else total + soft
        acc[...] += total
        g = jnp.concatenate(slopes, axis=1)
        d_row = lax.dot_general(g, p, NN, preferred_element_type=f32)
        dx[pl.ds(r0, V), :] = d_row if new_row else dx[pl.ds(r0, V), :] + d_row
        cut = width if new_col else 0 if add_col is None else add_col - c0
        for lo, hi, new in ((0, cut, True), (cut, width, False)):
            if lo < hi:
                d_col = lax.dot_general(g[:, lo:hi], x, TN, preferred_element_type=f32)
                at = pl.ds(c0 + lo, hi - lo)
                dp[at, :] = d_col if new else dp[at, :] + d_col

    C1, END = 512, 2 * V

    def cols(v, lo, hi, **new):
        tile(v, lo, hi - lo, **new)

    for h in (0, 1):
        wait("x", xs(3, 0), h)
        send_x(xs(3, 0), xs(2, 0), yu, h)
        wait("p", ps(3, 0), h)
        send_p(ps(3, 0), ps(2, 0), zu, h)
        wait("x", xs(0, 1), h)
        send_x(xs(0, 1), xs(1, 1), yd, h)
        wait("p", ps(0, 1), h)
        send_p(ps(0, 1), ps(1, 1), zd, h)
    for h in (0, 1):
        send_x(xs(0, 1), xs(3, 1), yu, h)
        send_p(ps(0, 1), ps(3, 1), zu, h)
    send_core((0, 1))
    send_core((3, 0))
    for h in (0, 1):
        wait("x", xs(1, 0), h)
    send_core((1, 0))
    for h in (0, 1):
        wait("p", ps(1, 0), h)
    col_info(4)
    col_info(6)
    rows_ready((0, 0))
    rows_ready((0, 1))
    cols(0, V, V + 384, new_row=True, new_col=True)
    for h in (0, 1):
        wait("x", xs(1, 1), h)
        send_x(xs(1, 1), xs(2, 1), yd, h)
        wait("p", ps(1, 1), h)
        send_p(ps(1, 1), ps(2, 1), zd, h)
        if h == 0:
            cols(0, V + 384, END, new_col=True)
    send_core((1, 1))
    for h in (0, 1):
        wait("x", xs(2, 0), h)
    send_core((2, 0))
    rows_ready((3, 0))
    rows_ready((1, 0))
    cols(1, V, END, new_row=True)
    rows_ready((2, 0))

    for h in (0, 1):
        wait("x", xs(2, 1), h)
    send_core((2, 1))
    for h in (0, 1):
        wait("x", xs(3, 1), h)
    send_core((3, 1))
    for u in ((2, 0), (2, 1), (3, 1)):
        for h in (0, 1):
            wait("p", ps(*u), h)
    col_info(0)
    col_info(2)
    rows_ready((2, 1))
    cols(3, 0, END, new_row=True, add_col=V)

    half = {}
    back = {}

    def to_core(u):
        half[u] = send(dx.at[rows(xs(*u, 1))], rc.at[XU.index(u)], cp)

    def add_core(u):
        half[u].wait_recv()
        dx[rows(xs(*u)), :] += rc[XU.index(u)]

    def send_dx(u, k, device, h):
        back["x", k, h] = send(dx.at[part(xs(*u), h)], ry.at[k, pl.ds(h * H, H)], device)

    def send_dp(u, k, device, h):
        back["p", k, h] = send(dp.at[part(ps(*u), h)], rz.at[k, pl.ds(h * H, H)], device)

    def add_dx(u, k, h):
        back["x", k, h].wait_recv()
        dx[part(xs(*u), h), :] += ry[k, pl.ds(h * H, H)]

    def add_dp(u, k, h):
        back["p", k, h].wait_recv()
        dp[part(ps(*u), h), :] += rz[k, pl.ds(h * H, H)]

    ring = {}

    def loss_send(k, peers):
        for n, peer in enumerate(peers):
            ring[k, n] = send(lsend.at[k], lrecv.at[3 * k + n], peer)

    def loss_add(k, n):
        for m in range(n):
            ring[k, m].wait_recv()
        if n == 1:
            lsend[k + 1] = lsend[k] + lrecv[3 * k]
        else:
            lsend[k + 1] = (lsend[k] + lrecv[3 * k]) + (lrecv[3 * k + 1] + lrecv[3 * k + 2])

    to_core((2, 0))
    to_core((2, 1))
    cols(0, 0, C1)
    add_core((2, 0))
    add_core((2, 1))
    for h in (0, 1):
        send_dx((2, 0), 0, yd, h)
        send_dx((2, 1), 1, yu, h)
    cols(1, 0, C1)
    rows_ready((3, 1))
    rows_ready((1, 1))
    cols(2, 0, C1, new_row=True)
    for h in (1, 0):
        send_dp((2, 0), 0, zd, h)
        send_dp((2, 1), 1, zu, h)
    cols(2, C1, END)
    to_core((1, 1))
    to_core((3, 1))
    send_dp((0, 1), 6, pxp, 1)
    cols(0, C1, V)
    add_core((1, 1))
    add_core((3, 1))
    send_dx((3, 1), 3, dxp, 1)
    send_dx((3, 1), 3, yd, 0)
    add_dx((1, 1), 1, 0)
    send_dx((1, 1), 5, yu, 0)
    cols(1, C1, V)
    lsend[0] = jnp.sum(acc[...], axis=0, keepdims=True)
    loss_send(0, (cp,))
    for u in ((3, 0), (1, 0), (0, 1), (0, 0)):
        to_core(u)
    add_dx((1, 1), 1, 1)
    send_dx((1, 1), 5, dxp, 1)
    add_dp((1, 1), 1, 1)
    send_dp((1, 1), 5, pxp, 1)
    send_dp((3, 1), 3, pxp, 1)
    loss_add(0, 1)
    loss_send(1, (zo, zu, zd))
    send_dp((3, 1), 3, zd, 0)
    send_dp((1, 0), 4, zu, 0)
    add_core((3, 0))
    add_dx((3, 0), 0, 0)
    add_core((1, 0))
    add_core((0, 1))
    add_core((0, 0))
    add_dx((3, 0), 0, 1)
    add_dp((3, 0), 0, 1)
    add_dp((1, 1), 1, 0)
    send_dp((1, 1), 5, zu, 0)
    add_dp((3, 0), 0, 0)
    send_dp((3, 0), 2, zd, 0)
    loss_add(1, 3)
    loss_send(2, (yo, yu, yd))
    send_dx((3, 0), 2, yd, 0)
    send_dx((1, 0), 4, yu, 0)
    add_dx((0, 1), 3, 0)
    add_dx((0, 1), 5, 0)
    loss_add(2, 3)
    loss_send(3, (xo, dxp, pxp))
    send_dx((0, 1), 6, dxp, 0)
    send_dx((0, 1), 6, dxp, 1)
    add_dx((3, 0), 3, 1)
    send_dx((3, 0), 2, yd, 1)
    add_dx((1, 0), 5, 1)
    send_dx((1, 0), 4, yu, 1)
    add_dp((1, 0), 5, 1)
    send_dp((1, 0), 4, zu, 1)
    add_dp((3, 0), 3, 1)
    send_dp((3, 0), 2, zd, 1)
    add_dp((0, 1), 3, 0)
    add_dp((0, 1), 5, 0)
    send_dp((0, 1), 6, pxp, 0)
    add_dx((0, 0), 2, 0)
    add_dx((0, 0), 4, 0)
    add_dp((0, 0), 6, 1)
    loss_add(3, 3)
    loss_ref[...] = lsend[4]
    add_dx((0, 0), 6, 0)
    add_dp((0, 0), 2, 0)
    add_dp((0, 0), 4, 0)
    add_dx((0, 0), 4, 1)
    add_dx((0, 0), 2, 1)
    add_dx((0, 0), 6, 1)
    sx_ref[...] = dx[rows(own_x), :]
    add_dp((0, 0), 4, 1)
    add_dp((0, 0), 2, 1)
    add_dp((0, 0), 6, 0)
    sp_ref[...] = dp[rows(own_p), :]
    for copy in pending:
        copy.wait_send()
    assert count[0] == N_SEM


def finish(x_ref, p_ref, sx_ref, sp_ref, sum_ref, loss_ref, gx_ref, gp_ref):
    for ref, sums, out in ((x_ref, sx_ref, gx_ref), (p_ref, sp_ref, gp_ref)):
        full, scale = normalize(ref)
        dnorm = sums[...]
        out[...] = scale * (dnorm - full * jnp.mean(dnorm * full, axis=-1, keepdims=True))
    n = float(128 * B)
    loss_ref[0] = jnp.sum(sum_ref[...]) * LN2 / (n * n)


def on_device(lensed, theta, region, match, gain, shift):
    vmem = pl.BlockSpec(memory_space=pltpu.VMEM)
    lensed, theta, region, match = (
        pltpu.with_memory_space_constraint(a, pltpu.HBM) for a in (lensed, theta, region.reshape(1, B), match.reshape(1, B))
    )
    smem = pl.BlockSpec(memory_space=pltpu.SMEM)
    block = jax.ShapeDtypeStruct((B, E), f32)
    half = jax.ShapeDtypeStruct((B, E), bf16)
    total, sum_x, sum_p, x, p = pl.pallas_call(
        kernel,
        out_shape=(jax.ShapeDtypeStruct((1, 128), f32), block, block, half, half),
        in_specs=[vmem] * 2 + [pl.BlockSpec(memory_space=pltpu.HBM)] * 4,
        out_specs=(vmem,) * 5,
        scratch_shapes=[
            pltpu.VMEM((B, E), bf16),
            pltpu.VMEM((B, E), bf16),
            pltpu.VMEM((1, B), i32),
            pltpu.VMEM((1, B), i32),
            pltpu.SemaphoreType.DMA((4,)),
            pltpu.VMEM((16 * B, E), bf16),
            pltpu.VMEM((8 * B, E), bf16),
            pltpu.VMEM((1, 1, 512), i32),
            pltpu.VMEM((16, 1, 256), i32),
            pltpu.VMEM((8, 1, 512), i32),
            pltpu.VMEM((16 * B, 128), i32),
            pltpu.VMEM((16 * B, 128), i32),
            pltpu.VMEM((1, 8 * B), i32),
            pltpu.VMEM((1, 8 * B), i32),
            pltpu.VMEM((16 * B, E), f32),
            pltpu.VMEM((8 * B, E), f32),
            pltpu.VMEM((8, B, E), f32),
            pltpu.VMEM((7, B, E), f32),
            pltpu.VMEM((7, B, E), f32),
            pltpu.VMEM((8, 128), f32),
            pltpu.VMEM((5, 1, 128), f32),
            pltpu.VMEM((12, 1, 128), f32),
            pltpu.SemaphoreType.DMA((N_SEM,)),
            pltpu.SemaphoreType.DMA((N_SEM,)),
        ],
        compiler_params=pltpu.CompilerParams(
            collective_id=0, has_side_effects=True, vmem_limit_bytes=48 << 20
        ),
        name="pairs",
    )(gain.reshape(1, 1), shift.reshape(1, 1), lensed, theta, region, match)
    return pl.pallas_call(
        finish,
        out_shape=(jax.ShapeDtypeStruct((1,), f32), block, block),
        in_specs=[vmem] * 5,
        out_specs=(smem, vmem, vmem),
        compiler_params=pltpu.CompilerParams(vmem_limit_bytes=8 << 20),
        name="finish",
    )(x, p, sum_x, sum_p, total)


def solution(mesh):
    both = ("row", "col")
    in_specs = (P(both, None), P(both, None), P(both), P(both), P(), P())
    out_specs = (P(), P(both, None), P(both, None))
    return jax.shard_map(
        on_device, mesh=mesh, in_specs=in_specs, out_specs=out_specs, check_vma=False
    )
```

```python
import jax
import jax.numpy as jnp
from jax import lax
from jax.experimental import pallas as pl
from jax.experimental.pallas import tpu as pltpu
from jax.sharding import PartitionSpec as P

f32 = jnp.float32
bf16 = jnp.bfloat16
i32 = jnp.int32
LOG2E = 1.4426950408889634
LN2 = 0.6931471805599453
MASKED = -1e5
NT = (((1,), (1,)), ((), ()))
NN = (((1,), (0,)), ((), ()))
TN = (((0,), (0,)), ((), ()))
MESH = pl.DeviceIdType.MESH
B = 192
E = 512
V = 4 * B
H = B // 2
XU = [(0, 0), (0, 1), (3, 0), (1, 0), (3, 1), (1, 1), (2, 0), (2, 1)]
PU = [(2, 0), (2, 1), (3, 1), (1, 1), (0, 0), (0, 1), (3, 0), (1, 0)]
N_SEM = 7 * 3 + 8 * 2 + 7 * 3 + 8 + 2 * 7 * 2 + 10


def xs(ry, rx, rc=0):
    return 2 * XU.index((ry, rx)) + rc


def ps(rz, rx):
    return PU.index((rz, rx))


def part(slot, h):
    return pl.ds(slot * B + h * H, H)


def rows(slot):
    return pl.ds(slot * B, B)


def pair_terms(s, row_region, row_match, col_region, col_index, gain, gain2, shift2):
    t = s * gain2 + shift2
    positive = row_match == col_index
    t = jnp.where(positive, -t, jnp.where(row_region != col_region, t, MASKED))
    soft = jnp.log2(1.0 + jnp.exp2(t))
    slope = jnp.exp2(t - soft) * jnp.where(positive, -gain, gain)
    return slope.astype(bf16), soft


def fold(x):
    return jnp.sum(x.reshape(x.shape[0] // 8, 8, 128), axis=0)


def normalize(ref):
    full = ref[...].astype(f32)
    scale = lax.rsqrt(jnp.mean(full * full, axis=-1, keepdims=True) + 1e-06)
    return full * scale, scale


def kernel(
    gain_ref, shift_ref, *hbm_and_rest,
):
    hbm, rest = hbm_and_rest[:4], hbm_and_rest[4:]
    pair_kernel(gain_ref, shift_ref, hbm, *rest)


def pair_kernel(
    gain_ref, shift_ref, hbm,
    loss_ref, sx_ref, sp_ref, xo_ref, po_ref,
    x_ref, p_ref, region_ref, match_ref, in_sem,
    xb, pb, lab_ref, lx, lp, rr, rm, cr, cj, dx, dp, rc, ry, rz, acc, lsend, lrecv, send_sem, recv_sem,
):
    r, c = lax.axis_index("row"), lax.axis_index("col")
    xl, z = r // 4, r % 4
    y, xh, core = c // 4, (c // 2) % 2, c % 2
    low = c % 4
    cp = (r, c + 1 - 2 * core)
    dxp = ((1 - xl) * 4 + z, c)
    pxp = ((1 - xl) * 4 + z, y * 4 + (1 - xh) * 2 + core)
    xo = (r, y * 4 + (1 - xh) * 2 + core)
    yu, yo, yd = ((r, ((y + k) % 4) * 4 + low) for k in (1, 2, 3))
    zu, zo, zd = ((xl * 4 + (z + k) % 4, c) for k in (1, 2, 3))

    count = [0]
    pending = []

    def send(src, dst, device):
        k = count[0]
        count[0] += 1
        copy = pltpu.make_async_remote_copy(
            src_ref=src, dst_ref=dst, send_sem=send_sem.at[k], recv_sem=recv_sem.at[k],
            device_id=device, device_id_type=MESH,
        )
        copy.start()
        pending.append(copy)
        return copy

    loads = [
        pltpu.make_async_copy(src, dst, in_sem.at[k])
        for k, (src, dst) in enumerate(zip(hbm, (x_ref, p_ref, region_ref, match_ref)))
    ]
    for load in loads:
        load.start()
    barrier = pltpu.get_barrier_semaphore()
    for peer in (cp, dxp, pxp, xo, yu, yo, yd, zu, zo, zd):
        pl.semaphore_signal(barrier, inc=1, device_id=peer, device_id_type=MESH)
    own_x, own_p = xs(0, 0), ps(0, 0)
    acc[...] = jnp.zeros_like(acc)
    for load in loads:
        load.wait()
    xb[rows(own_x), :] = normalize(x_ref)[0].astype(bf16)
    pb[rows(own_p), :] = normalize(p_ref)[0].astype(bf16)
    xo_ref[...] = x_ref[...]
    po_ref[...] = p_ref[...]
    packed = match_ref[...] * 64 + region_ref[...]
    wide = jnp.concatenate([packed, jnp.zeros((1, 64), i32)], axis=1)
    lab_ref[0] = jnp.concatenate([wide, pltpu.roll(wide, 64, 1)], axis=1)
    lx[own_x] = wide
    lp[own_p] = lab_ref[0]
    pl.semaphore_wait(barrier, 10)

    got = {}

    def send_x(src, dst, device, h):
        if h == 0:
            label = lab_ref.at[0, :, pl.ds(0, 256)] if src == own_x else lx.at[src]
            got["x", dst, "label"] = send(label, lx.at[dst], device)
        got["x", dst, h] = send(xb.at[part(src, h)], xb.at[part(dst, h)], device)

    def send_p(src, dst, device, h):
        if h == 0:
            label = lab_ref.at[0] if src == own_p else lp.at[src]
            got["p", dst, "label"] = send(label, lp.at[dst], device)
        got["p", dst, h] = send(pb.at[part(src, h)], pb.at[part(dst, h)], device)

    def wait(kind, slot, h):
        if h == 0:
            got[kind, slot, "label"].wait_recv()
        got[kind, slot, h].wait_recv()

    def send_core(u):
        src, dst = xs(*u), xs(*u, 1)
        label = lab_ref.at[0, :, pl.ds(0, 256)] if src == own_x else lx.at[src]
        got["core", u] = (send(label, lx.at[dst], cp), send(xb.at[rows(src)], xb.at[rows(dst)], cp))

    def row_info(slot):
        t = jnp.transpose(jnp.broadcast_to(lx[slot], (128, 256)))[0:B]
        rr[rows(slot), :] = t & 63
        rm[rows(slot), :] = t >> 6

    def rows_ready(u):
        row_info(xs(*u))
        for copy in got["core", u]:
            copy.wait_recv()
        row_info(xs(*u, 1))

    def base(rz_, rx):
        zz = (z + rz_) % 4
        if rx == 0:
            return ((xl * 4 + zz) * 16 + y * 4 + xh * 2 + core) * B
        return (((1 - xl) * 4 + zz) * 16 + y * 4 + (1 - xh) * 2 + core) * B

    def col_info(k0):
        first, second = lp[k0], lp[k0 + 1]
        base0, base1 = base(*PU[k0]), base(*PU[k0 + 1])
        lane = lax.broadcasted_iota(i32, (1, 128), 1)
        parts = (first[:, 0:128], first[:, 128:256] + second[:, 256:384], second[:, 384:512])
        for k in range(3):
            at = lane + k * 128
            cs = pl.ds(k0 * B + k * 128, 128)
            cr[:, cs] = parts[k] & 63
            cj[:, cs] = jnp.where(at < B, base0 + at, base1 + at - B)

    for h in (0, 1):
        send_x(own_x, xs(0, 1), dxp, h)
        send_p(own_p, ps(0, 1), pxp, h)
        send_x(own_x, xs(3, 0), yu, h)
        send_x(own_x, xs(1, 0), yd, h)
        send_p(own_p, ps(3, 0), zu, h)
        send_p(own_p, ps(1, 0), zd, h)
    send_core((0, 0))

    gain = gain_ref[...] / E
    gain2 = gain * LOG2E
    shift2 = shift_ref[...] * LOG2E

    def tile(v, c0, width, new_row=False, new_col=False, add_col=None):
        r0 = v * V
        x = xb[pl.ds(r0, V), :]
        p = pb[pl.ds(c0, width), :]
        s = lax.dot_general(x, p, NT, preferred_element_type=f32)
        region, match = rr[pl.ds(r0, V), :], rm[pl.ds(r0, V), :]
        slopes, total = [], None
        for k in range(width // 128):
            cs = pl.ds(c0 + k * 128, 128)
            slope, soft = pair_terms(
                s[:, k * 128 : (k + 1) * 128], region, match, cr[:, cs], cj[:, cs], gain, gain2, shift2
            )
            slopes.append(slope)
            soft = fold(soft)
            total = soft if total is None else total + soft
        acc[...] += total
        g = jnp.concatenate(slopes, axis=1)
        d_row = lax.dot_general(g, p, NN, preferred_element_type=f32)
        dx[pl.ds(r0, V), :] = d_row if new_row else dx[pl.ds(r0, V), :] + d_row
        cut = width if new_col else 0 if add_col is None else add_col - c0
        for lo, hi, new in ((0, cut, True), (cut, width, False)):
            if lo < hi:
                d_col = lax.dot_general(g[:, lo:hi], x, TN, preferred_element_type=f32)
                at = pl.ds(c0 + lo, hi - lo)
                dp[at, :] = d_col if new else dp[at, :] + d_col

    C1, END = 512, 2 * V

    def cols(v, lo, hi, **new):
        tile(v, lo, hi - lo, **new)

    for h in (0, 1):
        wait("x", xs(3, 0), h)
        send_x(xs(3, 0), xs(2, 0), yu, h)
        wait("p", ps(3, 0), h)
        send_p(ps(3, 0), ps(2, 0), zu, h)
        wait("x", xs(0, 1), h)
        send_x(xs(0, 1), xs(1, 1), yd, h)
        wait("p", ps(0, 1), h)
        send_p(ps(0, 1), ps(1, 1), zd, h)
    for h in (0, 1):
        send_x(xs(0, 1), xs(3, 1), yu, h)
        send_p(ps(0, 1), ps(3, 1), zu, h)
    send_core((0, 1))
    send_core((3, 0))
    for h in (0, 1):
        wait("x", xs(1, 0), h)
    send_core((1, 0))
    for h in (0, 1):
        wait("p", ps(1, 0), h)
    col_info(4)
    col_info(6)
    rows_ready((0, 0))
    rows_ready((0, 1))
    cols(0, V, V + 384, new_row=True, new_col=True)
    for h in (0, 1):
        wait("x", xs(1, 1), h)
        send_x(xs(1, 1), xs(2, 1), yd, h)
        wait("p", ps(1, 1), h)
        send_p(ps(1, 1), ps(2, 1), zd, h)
        if h == 0:
            cols(0, V + 384, END, new_col=True)
    send_core((1, 1))
    for h in (0, 1):
        wait("x", xs(2, 0), h)
    send_core((2, 0))
    rows_ready((3, 0))
    rows_ready((1, 0))
    cols(1, V, END, new_row=True)
    rows_ready((2, 0))

    for h in (0, 1):
        wait("x", xs(2, 1), h)
    send_core((2, 1))
    for h in (0, 1):
        wait("x", xs(3, 1), h)
    send_core((3, 1))
    for u in ((2, 0), (2, 1), (3, 1)):
        for h in (0, 1):
            wait("p", ps(*u), h)
    col_info(0)
    col_info(2)
    rows_ready((2, 1))
    cols(3, 0, END, new_row=True, add_col=V)

    half = {}
    back = {}

    def to_core(u):
        half[u] = send(dx.at[rows(xs(*u, 1))], rc.at[XU.index(u)], cp)

    def add_core(u):
        half[u].wait_recv()
        dx[rows(xs(*u)), :] += rc[XU.index(u)]

    def send_dx(u, k, device, h):
        back["x", k, h] = send(dx.at[part(xs(*u), h)], ry.at[k, pl.ds(h * H, H)], device)

    def send_dp(u, k, device, h):
        back["p", k, h] = send(dp.at[part(ps(*u), h)], rz.at[k, pl.ds(h * H, H)], device)

    def add_dx(u, k, h):
        back["x", k, h].wait_recv()
        dx[part(xs(*u), h), :] += ry[k, pl.ds(h * H, H)]

    def add_dp(u, k, h):
        back["p", k, h].wait_recv()
        dp[part(ps(*u), h), :] += rz[k, pl.ds(h * H, H)]

    ring = {}

    def loss_send(k, peers):
        for n, peer in enumerate(peers):
            ring[k, n] = send(lsend.at[k], lrecv.at[3 * k + n], peer)

    def loss_add(k, n):
        for m in range(n):
            ring[k, m].wait_recv()
        if n == 1:
            lsend[k + 1] = lsend[k] + lrecv[3 * k]
        else:
            lsend[k + 1] = (lsend[k] + lrecv[3 * k]) + (lrecv[3 * k + 1] + lrecv[3 * k + 2])

    to_core((2, 0))
    to_core((2, 1))
    cols(0, 0, C1)
    add_core((2, 0))
    add_core((2, 1))
    for h in (0, 1):
        send_dx((2, 0), 0, yd, h)
        send_dx((2, 1), 1, yu, h)
    cols(1, 0, C1)
    rows_ready((3, 1))
    rows_ready((1, 1))
    cols(2, 0, C1, new_row=True)
    for h in (0, 1):
        send_dp((2, 0), 0, zd, h)
        send_dp((2, 1), 1, zu, h)
    cols(2, C1, END)
    to_core((1, 1))
    to_core((3, 1))
    send_dp((0, 1), 6, pxp, 1)
    cols(0, C1, V)
    add_core((1, 1))
    add_core((3, 1))
    send_dx((3, 1), 3, dxp, 1)
    send_dx((3, 1), 3, yd, 0)
    add_dx((1, 1), 1, 0)
    send_dx((1, 1), 5, yu, 0)
    cols(1, C1, V)
    lsend[0] = jnp.sum(acc[...], axis=0, keepdims=True)
    loss_send(0, (cp,))
    for u in ((3, 0), (1, 0), (0, 1), (0, 0)):
        to_core(u)
    add_dx((1, 1), 1, 1)
    send_dx((1, 1), 5, dxp, 1)
    send_dp((3, 1), 3, pxp, 1)
    loss_add(0, 1)
    loss_send(1, (zo, zu, zd))
    send_dp((3, 1), 3, zd, 0)
    add_dp((1, 1), 1, 0)
    send_dp((1, 1), 5, zu, 0)
    add_dp((3, 0), 0, 0)
    send_dp((3, 0), 2, zd, 0)
    send_dp((1, 0), 4, zu, 0)
    add_core((3, 0))
    add_dx((3, 0), 0, 0)
    add_core((1, 0))
    add_core((0, 1))
    add_core((0, 0))
    add_dx((3, 0), 0, 1)
    add_dp((1, 1), 1, 1)
    send_dp((1, 1), 5, pxp, 1)
    add_dp((3, 0), 0, 1)
    loss_add(1, 3)
    loss_send(2, (yo, yu, yd))
    send_dx((3, 0), 2, yd, 0)
    send_dx((1, 0), 4, yu, 0)
    add_dx((0, 1), 3, 0)
    add_dx((0, 1), 5, 0)
    send_dx((0, 1), 6, dxp, 0)
    add_dx((3, 0), 3, 1)
    send_dx((3, 0), 2, yd, 1)
    add_dp((3, 0), 3, 1)
    send_dp((3, 0), 2, zd, 1)
    loss_add(2, 3)
    loss_send(3, (xo, dxp, pxp))
    send_dx((0, 1), 6, dxp, 1)
    add_dx((1, 0), 5, 1)
    send_dx((1, 0), 4, yu, 1)
    add_dp((0, 1), 3, 0)
    add_dp((0, 1), 5, 0)
    send_dp((0, 1), 6, pxp, 0)
    add_dp((1, 0), 5, 1)
    send_dp((1, 0), 4, zu, 1)
    add_dx((0, 0), 2, 0)
    add_dx((0, 0), 4, 0)
    add_dp((0, 0), 6, 1)
    loss_add(3, 3)
    loss_ref[...] = lsend[4]
    add_dx((0, 0), 6, 0)
    add_dp((0, 0), 2, 0)
    add_dp((0, 0), 4, 0)
    add_dx((0, 0), 4, 1)
    add_dx((0, 0), 2, 1)
    add_dx((0, 0), 6, 1)
    sx_ref[...] = dx[rows(own_x), :]
    add_dp((0, 0), 4, 1)
    add_dp((0, 0), 2, 1)
    add_dp((0, 0), 6, 0)
    sp_ref[...] = dp[rows(own_p), :]
    for copy in pending:
        copy.wait_send()
    assert count[0] == N_SEM


def finish(x_ref, p_ref, sx_ref, sp_ref, sum_ref, loss_ref, gx_ref, gp_ref):
    for ref, sums, out in ((x_ref, sx_ref, gx_ref), (p_ref, sp_ref, gp_ref)):
        full, scale = normalize(ref)
        dnorm = sums[...]
        out[...] = scale * (dnorm - full * jnp.mean(dnorm * full, axis=-1, keepdims=True))
    n = float(128 * B)
    loss_ref[0] = jnp.sum(sum_ref[...]) * LN2 / (n * n)


def on_device(lensed, theta, region, match, gain, shift):
    vmem = pl.BlockSpec(memory_space=pltpu.VMEM)
    lensed, theta, region, match = (
        pltpu.with_memory_space_constraint(a, pltpu.HBM) for a in (lensed, theta, region.reshape(1, B), match.reshape(1, B))
    )
    smem = pl.BlockSpec(memory_space=pltpu.SMEM)
    block = jax.ShapeDtypeStruct((B, E), f32)
    half = jax.ShapeDtypeStruct((B, E), bf16)
    total, sum_x, sum_p, x, p = pl.pallas_call(
        kernel,
        out_shape=(jax.ShapeDtypeStruct((1, 128), f32), block, block, half, half),
        in_specs=[vmem] * 2 + [pl.BlockSpec(memory_space=pltpu.HBM)] * 4,
        out_specs=(vmem,) * 5,
        scratch_shapes=[
            pltpu.VMEM((B, E), bf16),
            pltpu.VMEM((B, E), bf16),
            pltpu.VMEM((1, B), i32),
            pltpu.VMEM((1, B), i32),
            pltpu.SemaphoreType.DMA((4,)),
            pltpu.VMEM((16 * B, E), bf16),
            pltpu.VMEM((8 * B, E), bf16),
            pltpu.VMEM((1, 1, 512), i32),
            pltpu.VMEM((16, 1, 256), i32),
            pltpu.VMEM((8, 1, 512), i32),
            pltpu.VMEM((16 * B, 128), i32),
            pltpu.VMEM((16 * B, 128), i32),
            pltpu.VMEM((1, 8 * B), i32),
            pltpu.VMEM((1, 8 * B), i32),
            pltpu.VMEM((16 * B, E), f32),
            pltpu.VMEM((8 * B, E), f32),
            pltpu.VMEM((8, B, E), f32),
            pltpu.VMEM((7, B, E), f32),
            pltpu.VMEM((7, B, E), f32),
            pltpu.VMEM((8, 128), f32),
            pltpu.VMEM((5, 1, 128), f32),
            pltpu.VMEM((12, 1, 128), f32),
            pltpu.SemaphoreType.DMA((N_SEM,)),
            pltpu.SemaphoreType.DMA((N_SEM,)),
        ],
        compiler_params=pltpu.CompilerParams(
            collective_id=0, has_side_effects=True, vmem_limit_bytes=48 << 20
        ),
        name="pairs",
    )(gain.reshape(1, 1), shift.reshape(1, 1), lensed, theta, region, match)
    return pl.pallas_call(
        finish,
        out_shape=(jax.ShapeDtypeStruct((1,), f32), block, block),
        in_specs=[vmem] * 5,
        out_specs=(smem, vmem, vmem),
        compiler_params=pltpu.CompilerParams(vmem_limit_bytes=8 << 20),
        name="finish",
    )(x, p, sum_x, sum_p, total)


def solution(mesh):
    both = ("row", "col")
    in_specs = (P(both, None), P(both, None), P(both), P(both), P(), P())
    out_specs = (P(), P(both, None), P(both, None))
    return jax.shard_map(
        on_device, mesh=mesh, in_specs=in_specs, out_specs=out_specs, check_vma=False
    )
```

```python
import jax
import jax.numpy as jnp
from jax import lax
from jax.experimental import pallas as pl
from jax.experimental.pallas import tpu as pltpu
from jax.sharding import PartitionSpec as P

f32 = jnp.float32
bf16 = jnp.bfloat16
i32 = jnp.int32
LOG2E = 1.4426950408889634
LN2 = 0.6931471805599453
MASKED = -1e5
NT = (((1,), (1,)), ((), ()))
NN = (((1,), (0,)), ((), ()))
TN = (((0,), (0,)), ((), ()))
MESH = pl.DeviceIdType.MESH
B = 192
E = 512
V = 4 * B
H = B // 2
CUT_X, CUT_P = 112, 112
XU = [(0, 0), (0, 1), (3, 0), (1, 0), (3, 1), (1, 1), (2, 0), (2, 1)]
PU = [(2, 0), (2, 1), (3, 1), (1, 1), (0, 0), (0, 1), (3, 0), (1, 0)]
N_SEM = 7 * 3 + 8 * 2 + 7 * 3 + 8 + 2 * 7 * 2 + 10


def xs(ry, rx, rc=0):
    return 2 * XU.index((ry, rx)) + rc


def ps(rz, rx):
    return PU.index((rz, rx))


def part(slot, h):
    return pl.ds(slot * B + h * H, H)


def rows(slot):
    return pl.ds(slot * B, B)


def pair_terms(s, row_region, row_match, col_region, col_index, gain, gain2, shift2):
    t = s * gain2 + shift2
    positive = row_match == col_index
    t = jnp.where(positive, -t, jnp.where(row_region != col_region, t, MASKED))
    soft = jnp.log2(1.0 + jnp.exp2(t))
    slope = jnp.exp2(t - soft) * jnp.where(positive, -gain, gain)
    return slope.astype(bf16), soft


def fold(x):
    return jnp.sum(x.reshape(x.shape[0] // 8, 8, 128), axis=0)


def normalize(ref):
    full = ref[...].astype(f32)
    scale = lax.rsqrt(jnp.mean(full * full, axis=-1, keepdims=True) + 1e-06)
    return full * scale, scale


def kernel(
    gain_ref, shift_ref, *hbm_and_rest,
):
    hbm, rest = hbm_and_rest[:4], hbm_and_rest[4:]
    pair_kernel(gain_ref, shift_ref, hbm, *rest)


def pair_kernel(
    gain_ref, shift_ref, hbm,
    loss_ref, sx_ref, sp_ref, xo_ref, po_ref,
    x_ref, p_ref, region_ref, match_ref, in_sem,
    xb, pb, lab_ref, lx, lp, rr, rm, cr, cj, dx, dp, rc, ry, rz, acc, lsend, lrecv, send_sem, recv_sem,
):
    r, c = lax.axis_index("row"), lax.axis_index("col")
    xl, z = r // 4, r % 4
    y, xh, core = c // 4, (c // 2) % 2, c % 2
    low = c % 4
    cp = (r, c + 1 - 2 * core)
    dxp = ((1 - xl) * 4 + z, c)
    pxp = ((1 - xl) * 4 + z, y * 4 + (1 - xh) * 2 + core)
    xo = (r, y * 4 + (1 - xh) * 2 + core)
    yu, yo, yd = ((r, ((y + k) % 4) * 4 + low) for k in (1, 2, 3))
    zu, zo, zd = ((xl * 4 + (z + k) % 4, c) for k in (1, 2, 3))

    count = [0]
    pending = []

    def send(src, dst, device):
        k = count[0]
        count[0] += 1
        copy = pltpu.make_async_remote_copy(
            src_ref=src, dst_ref=dst, send_sem=send_sem.at[k], recv_sem=recv_sem.at[k],
            device_id=device, device_id_type=MESH,
        )
        copy.start()
        pending.append(copy)
        return copy

    loads = [
        pltpu.make_async_copy(src, dst, in_sem.at[k])
        for k, (src, dst) in enumerate(zip(hbm, (x_ref, p_ref, region_ref, match_ref)))
    ]
    for load in loads:
        load.start()
    barrier = pltpu.get_barrier_semaphore()
    for peer in (cp, dxp, pxp, xo, yu, yo, yd, zu, zo, zd):
        pl.semaphore_signal(barrier, inc=1, device_id=peer, device_id_type=MESH)
    own_x, own_p = xs(0, 0), ps(0, 0)
    acc[...] = jnp.zeros_like(acc)
    for load in loads:
        load.wait()
    xb[rows(own_x), :] = normalize(x_ref)[0].astype(bf16)
    pb[rows(own_p), :] = normalize(p_ref)[0].astype(bf16)
    xo_ref[...] = x_ref[...]
    po_ref[...] = p_ref[...]
    packed = match_ref[...] * 64 + region_ref[...]
    wide = jnp.concatenate([packed, jnp.zeros((1, 64), i32)], axis=1)
    lab_ref[0] = jnp.concatenate([wide, pltpu.roll(wide, 64, 1)], axis=1)
    lx[own_x] = wide
    lp[own_p] = lab_ref[0]
    pl.semaphore_wait(barrier, 10)

    got = {}

    def send_x(src, dst, device, h):
        if h == 0:
            label = lab_ref.at[0, :, pl.ds(0, 256)] if src == own_x else lx.at[src]
            got["x", dst, "label"] = send(label, lx.at[dst], device)
        got["x", dst, h] = send(xb.at[part(src, h)], xb.at[part(dst, h)], device)

    def send_p(src, dst, device, h):
        if h == 0:
            label = lab_ref.at[0] if src == own_p else lp.at[src]
            got["p", dst, "label"] = send(label, lp.at[dst], device)
        got["p", dst, h] = send(pb.at[part(src, h)], pb.at[part(dst, h)], device)

    def wait(kind, slot, h):
        if h == 0:
            got[kind, slot, "label"].wait_recv()
        got[kind, slot, h].wait_recv()

    def send_core(u):
        src, dst = xs(*u), xs(*u, 1)
        label = lab_ref.at[0, :, pl.ds(0, 256)] if src == own_x else lx.at[src]
        got["core", u] = (send(label, lx.at[dst], cp), send(xb.at[rows(src)], xb.at[rows(dst)], cp))

    def row_info(slot):
        t = jnp.transpose(jnp.broadcast_to(lx[slot], (128, 256)))[0:B]
        rr[rows(slot), :] = t & 63
        rm[rows(slot), :] = t >> 6

    def rows_ready(u):
        row_info(xs(*u))
        for copy in got["core", u]:
            copy.wait_recv()
        row_info(xs(*u, 1))

    def base(rz_, rx):
        zz = (z + rz_) % 4
        if rx == 0:
            return ((xl * 4 + zz) * 16 + y * 4 + xh * 2 + core) * B
        return (((1 - xl) * 4 + zz) * 16 + y * 4 + (1 - xh) * 2 + core) * B

    def col_info(k0):
        first, second = lp[k0], lp[k0 + 1]
        base0, base1 = base(*PU[k0]), base(*PU[k0 + 1])
        lane = lax.broadcasted_iota(i32, (1, 128), 1)
        parts = (first[:, 0:128], first[:, 128:256] + second[:, 256:384], second[:, 384:512])
        for k in range(3):
            at = lane + k * 128
            cs = pl.ds(k0 * B + k * 128, 128)
            cr[:, cs] = parts[k] & 63
            cj[:, cs] = jnp.where(at < B, base0 + at, base1 + at - B)

    for h in (0, 1):
        send_x(own_x, xs(0, 1), dxp, h)
        send_p(own_p, ps(0, 1), pxp, h)
        send_x(own_x, xs(3, 0), yu, h)
        send_x(own_x, xs(1, 0), yd, h)
        send_p(own_p, ps(3, 0), zu, h)
        send_p(own_p, ps(1, 0), zd, h)
    send_core((0, 0))

    gain = gain_ref[...] / E
    gain2 = gain * LOG2E
    shift2 = shift_ref[...] * LOG2E

    def tile(v, c0, width, new_row=False, new_col=False, add_col=None):
        r0 = v * V
        x = xb[pl.ds(r0, V), :]
        p = pb[pl.ds(c0, width), :]
        s = lax.dot_general(x, p, NT, preferred_element_type=f32)
        region, match = rr[pl.ds(r0, V), :], rm[pl.ds(r0, V), :]
        slopes, total = [], None
        for k in range(width // 128):
            cs = pl.ds(c0 + k * 128, 128)
            slope, soft = pair_terms(
                s[:, k * 128 : (k + 1) * 128], region, match, cr[:, cs], cj[:, cs], gain, gain2, shift2
            )
            slopes.append(slope)
            soft = fold(soft)
            total = soft if total is None else total + soft
        acc[...] += total
        g = jnp.concatenate(slopes, axis=1)
        d_row = lax.dot_general(g, p, NN, preferred_element_type=f32)
        dx[pl.ds(r0, V), :] = d_row if new_row else dx[pl.ds(r0, V), :] + d_row
        cut = width if new_col else 0 if add_col is None else add_col - c0
        for lo, hi, new in ((0, cut, True), (cut, width, False)):
            if lo < hi:
                d_col = lax.dot_general(g[:, lo:hi], x, TN, preferred_element_type=f32)
                at = pl.ds(c0 + lo, hi - lo)
                dp[at, :] = d_col if new else dp[at, :] + d_col

    C1, END = 512, 2 * V

    def cols(v, lo, hi, **new):
        tile(v, lo, hi - lo, **new)

    for h in (0, 1):
        wait("x", xs(3, 0), h)
        send_x(xs(3, 0), xs(2, 0), yu, h)
        wait("p", ps(3, 0), h)
        send_p(ps(3, 0), ps(2, 0), zu, h)
        wait("x", xs(0, 1), h)
        send_x(xs(0, 1), xs(1, 1), yd, h)
        wait("p", ps(0, 1), h)
        send_p(ps(0, 1), ps(1, 1), zd, h)
    for h in (0, 1):
        send_x(xs(0, 1), xs(3, 1), yu, h)
        send_p(ps(0, 1), ps(3, 1), zu, h)
    send_core((0, 1))
    send_core((3, 0))
    for h in (0, 1):
        wait("x", xs(1, 0), h)
    send_core((1, 0))
    for h in (0, 1):
        wait("p", ps(1, 0), h)
    col_info(4)
    col_info(6)
    rows_ready((0, 0))
    rows_ready((0, 1))
    cols(0, V, V + 384, new_row=True, new_col=True)
    for h in (0, 1):
        wait("x", xs(1, 1), h)
        send_x(xs(1, 1), xs(2, 1), yd, h)
        wait("p", ps(1, 1), h)
        send_p(ps(1, 1), ps(2, 1), zd, h)
        if h == 0:
            cols(0, V + 384, END, new_col=True)
    send_core((1, 1))
    for h in (0, 1):
        wait("x", xs(2, 0), h)
    send_core((2, 0))
    rows_ready((3, 0))
    rows_ready((1, 0))
    cols(1, V, END, new_row=True)
    rows_ready((2, 0))

    for h in (0, 1):
        wait("x", xs(2, 1), h)
    send_core((2, 1))
    for h in (0, 1):
        wait("x", xs(3, 1), h)
    send_core((3, 1))
    for u in ((2, 0), (2, 1), (3, 1)):
        for h in (0, 1):
            wait("p", ps(*u), h)
    col_info(0)
    col_info(2)
    rows_ready((2, 1))
    cols(3, 0, END, new_row=True, add_col=V)

    half = {}
    back = {}

    def to_core(u):
        half[u] = send(dx.at[rows(xs(*u, 1))], rc.at[XU.index(u)], cp)

    def add_core(u):
        half[u].wait_recv()
        dx[rows(xs(*u)), :] += rc[XU.index(u)]

    def cut(slot, h, first):
        return pl.ds(slot * B + h * first, B - first if h else first)

    def send_dx(u, k, device, h):
        back["x", k, h] = send(dx.at[cut(xs(*u), h, CUT_X)], ry.at[k, cut(0, h, CUT_X)], device)

    def send_dp(u, k, device, h):
        back["p", k, h] = send(dp.at[cut(ps(*u), h, CUT_P)], rz.at[k, cut(0, h, CUT_P)], device)

    def add_dx(u, k, h):
        back["x", k, h].wait_recv()
        dx[cut(xs(*u), h, CUT_X), :] += ry[k, cut(0, h, CUT_X)]

    def add_dp(u, k, h):
        back["p", k, h].wait_recv()
        dp[cut(ps(*u), h, CUT_P), :] += rz[k, cut(0, h, CUT_P)]

    ring = {}

    def loss_send(k, peers):
        for n, peer in enumerate(peers):
            ring[k, n] = send(lsend.at[k], lrecv.at[3 * k + n], peer)

    def loss_add(k, n):
        for m in range(n):
            ring[k, m].wait_recv()
        if n == 1:
            lsend[k + 1] = lsend[k] + lrecv[3 * k]
        else:
            lsend[k + 1] = (lsend[k] + lrecv[3 * k]) + (lrecv[3 * k + 1] + lrecv[3 * k + 2])

    to_core((2, 0))
    to_core((2, 1))
    cols(0, 0, C1)
    add_core((2, 0))
    add_core((2, 1))
    for h in (0, 1):
        send_dx((2, 0), 0, yd, h)
        send_dx((2, 1), 1, yu, h)
    cols(1, 0, C1)
    rows_ready((3, 1))
    rows_ready((1, 1))
    cols(2, 0, C1, new_row=True)
    for h in (0, 1):
        send_dp((2, 0), 0, zd, h)
        send_dp((2, 1), 1, zu, h)
    cols(2, C1, END)
    to_core((1, 1))
    to_core((3, 1))
    send_dp((0, 1), 6, pxp, 1)
    cols(0, C1, V)
    add_core((1, 1))
    add_core((3, 1))
    send_dx((3, 1), 3, dxp, 1)
    send_dx((3, 1), 3, yd, 0)
    add_dx((1, 1), 1, 0)
    send_dx((1, 1), 5, yu, 0)
    cols(1, C1, V)
    lsend[0] = jnp.sum(acc[...], axis=0, keepdims=True)
    loss_send(0, (cp,))
    for u in ((3, 0), (1, 0), (0, 1), (0, 0)):
        to_core(u)
    add_dx((1, 1), 1, 1)
    send_dx((1, 1), 5, dxp, 1)
    send_dp((3, 1), 3, pxp, 1)
    loss_add(0, 1)
    loss_send(1, (zo, zu, zd))
    send_dp((3, 1), 3, zd, 0)
    add_dp((1, 1), 1, 0)
    send_dp((1, 1), 5, zu, 0)
    add_dp((3, 0), 0, 0)
    send_dp((3, 0), 2, zd, 0)
    send_dp((1, 0), 4, zu, 0)
    add_core((3, 0))
    add_dx((3, 0), 0, 0)
    add_core((1, 0))
    add_core((0, 1))
    add_core((0, 0))
    add_dx((3, 0), 0, 1)
    add_dp((1, 1), 1, 1)
    send_dp((1, 1), 5, pxp, 1)
    add_dp((3, 0), 0, 1)
    loss_add(1, 3)
    loss_send(2, (yo, yu, yd))
    send_dx((3, 0), 2, yd, 0)
    send_dx((1, 0), 4, yu, 0)
    add_dx((0, 1), 3, 0)
    add_dx((0, 1), 5, 0)
    send_dx((0, 1), 6, dxp, 0)
    add_dx((3, 0), 3, 1)
    send_dx((3, 0), 2, yd, 1)
    add_dp((3, 0), 3, 1)
    send_dp((3, 0), 2, zd, 1)
    loss_add(2, 3)
    loss_send(3, (xo, dxp, pxp))
    send_dx((0, 1), 6, dxp, 1)
    add_dx((1, 0), 5, 1)
    send_dx((1, 0), 4, yu, 1)
    add_dp((0, 1), 3, 0)
    add_dp((0, 1), 5, 0)
    send_dp((0, 1), 6, pxp, 0)
    add_dp((1, 0), 5, 1)
    send_dp((1, 0), 4, zu, 1)
    add_dx((0, 0), 2, 0)
    add_dx((0, 0), 4, 0)
    add_dp((0, 0), 6, 1)
    loss_add(3, 3)
    loss_ref[...] = lsend[4]
    add_dx((0, 0), 6, 0)
    add_dp((0, 0), 2, 0)
    add_dp((0, 0), 4, 0)
    add_dx((0, 0), 4, 1)
    add_dx((0, 0), 2, 1)
    add_dx((0, 0), 6, 1)
    sx_ref[...] = dx[rows(own_x), :]
    add_dp((0, 0), 4, 1)
    add_dp((0, 0), 2, 1)
    add_dp((0, 0), 6, 0)
    sp_ref[...] = dp[rows(own_p), :]
    for copy in pending:
        copy.wait_send()
    assert count[0] == N_SEM


def finish(x_ref, p_ref, sx_ref, sp_ref, sum_ref, loss_ref, gx_ref, gp_ref):
    for ref, sums, out in ((x_ref, sx_ref, gx_ref), (p_ref, sp_ref, gp_ref)):
        full, scale = normalize(ref)
        dnorm = sums[...]
        out[...] = scale * (dnorm - full * jnp.mean(dnorm * full, axis=-1, keepdims=True))
    n = float(128 * B)
    loss_ref[0] = jnp.sum(sum_ref[...]) * LN2 / (n * n)


def on_device(lensed, theta, region, match, gain, shift):
    vmem = pl.BlockSpec(memory_space=pltpu.VMEM)
    lensed, theta, region, match = (
        pltpu.with_memory_space_constraint(a, pltpu.HBM) for a in (lensed, theta, region.reshape(1, B), match.reshape(1, B))
    )
    smem = pl.BlockSpec(memory_space=pltpu.SMEM)
    block = jax.ShapeDtypeStruct((B, E), f32)
    half = jax.ShapeDtypeStruct((B, E), bf16)
    total, sum_x, sum_p, x, p = pl.pallas_call(
        kernel,
        out_shape=(jax.ShapeDtypeStruct((1, 128), f32), block, block, half, half),
        in_specs=[vmem] * 2 + [pl.BlockSpec(memory_space=pltpu.HBM)] * 4,
        out_specs=(vmem,) * 5,
        scratch_shapes=[
            pltpu.VMEM((B, E), bf16),
            pltpu.VMEM((B, E), bf16),
            pltpu.VMEM((1, B), i32),
            pltpu.VMEM((1, B), i32),
            pltpu.SemaphoreType.DMA((4,)),
            pltpu.VMEM((16 * B, E), bf16),
            pltpu.VMEM((8 * B, E), bf16),
            pltpu.VMEM((1, 1, 512), i32),
            pltpu.VMEM((16, 1, 256), i32),
            pltpu.VMEM((8, 1, 512), i32),
            pltpu.VMEM((16 * B, 128), i32),
            pltpu.VMEM((16 * B, 128), i32),
            pltpu.VMEM((1, 8 * B), i32),
            pltpu.VMEM((1, 8 * B), i32),
            pltpu.VMEM((16 * B, E), f32),
            pltpu.VMEM((8 * B, E), f32),
            pltpu.VMEM((8, B, E), f32),
            pltpu.VMEM((7, B, E), f32),
            pltpu.VMEM((7, B, E), f32),
            pltpu.VMEM((8, 128), f32),
            pltpu.VMEM((5, 1, 128), f32),
            pltpu.VMEM((12, 1, 128), f32),
            pltpu.SemaphoreType.DMA((N_SEM,)),
            pltpu.SemaphoreType.DMA((N_SEM,)),
        ],
        compiler_params=pltpu.CompilerParams(
            collective_id=0, has_side_effects=True, vmem_limit_bytes=48 << 20
        ),
        name="pairs",
    )(gain.reshape(1, 1), shift.reshape(1, 1), lensed, theta, region, match)
    return pl.pallas_call(
        finish,
        out_shape=(jax.ShapeDtypeStruct((1,), f32), block, block),
        in_specs=[vmem] * 5,
        out_specs=(smem, vmem, vmem),
        compiler_params=pltpu.CompilerParams(vmem_limit_bytes=8 << 20),
        name="finish",
    )(x, p, sum_x, sum_p, total)


def solution(mesh):
    both = ("row", "col")
    in_specs = (P(both, None), P(both, None), P(both), P(both), P(), P())
    out_specs = (P(), P(both, None), P(both, None))
    return jax.shard_map(
        on_device, mesh=mesh, in_specs=in_specs, out_specs=out_specs, check_vma=False
    )
```

```python
import jax
import jax.numpy as jnp
from jax import lax
from jax.experimental import pallas as pl
from jax.experimental.pallas import tpu as pltpu
from jax.sharding import PartitionSpec as P

f32 = jnp.float32
bf16 = jnp.bfloat16
i32 = jnp.int32
LOG2E = 1.4426950408889634
LN2 = 0.6931471805599453
MASKED = -1e5
NT = (((1,), (1,)), ((), ()))
NN = (((1,), (0,)), ((), ()))
TN = (((0,), (0,)), ((), ()))
MESH = pl.DeviceIdType.MESH
B = 192
E = 512
V = 4 * B
H = B // 2
CUT_X, CUT_P = 112, 112
XU = [(0, 0), (0, 1), (3, 0), (1, 0), (3, 1), (1, 1), (2, 0), (2, 1)]
PU = [(2, 0), (2, 1), (3, 1), (1, 1), (0, 0), (0, 1), (3, 0), (1, 0)]
N_SEM = 7 * 3 + 8 * 2 + 7 * 3 + 8 + 2 * 7 * 2 + 10


def xs(ry, rx, rc=0):
    return 2 * XU.index((ry, rx)) + rc


def ps(rz, rx):
    return PU.index((rz, rx))


def part(slot, h):
    return pl.ds(slot * B + h * H, H)


def rows(slot):
    return pl.ds(slot * B, B)


def pair_terms(s, row_region, row_match, col_region, col_index, gain, gain2, shift2):
    t = s * gain2 + shift2
    positive = row_match == col_index
    t = jnp.where(positive, -t, jnp.where(row_region != col_region, t, MASKED))
    soft = jnp.log2(1.0 + jnp.exp2(t))
    slope = jnp.exp2(t - soft) * jnp.where(positive, -gain, gain)
    return slope.astype(bf16), soft


def fold(x):
    return jnp.sum(x.reshape(x.shape[0] // 8, 8, 128), axis=0)


def normalize(ref):
    full = ref[...].astype(f32)
    scale = lax.rsqrt(jnp.mean(full * full, axis=-1, keepdims=True) + 1e-06)
    return full * scale, scale


def kernel(
    gain_ref, shift_ref, *hbm_and_rest,
):
    hbm, rest = hbm_and_rest[:4], hbm_and_rest[4:]
    pair_kernel(gain_ref, shift_ref, hbm, *rest)


def pair_kernel(
    gain_ref, shift_ref, hbm,
    loss_ref, sx_ref, sp_ref, xo_ref, po_ref,
    x_ref, p_ref, region_ref, match_ref, in_sem,
    xb, pb, lab_ref, lx, lp, rr, rm, cr, cj, dx, dp, rc, ry, rz, acc, lsend, lrecv, send_sem, recv_sem,
):
    r, c = lax.axis_index("row"), lax.axis_index("col")
    xl, z = r // 4, r % 4
    y, xh, core = c // 4, (c // 2) % 2, c % 2
    low = c % 4
    cp = (r, c + 1 - 2 * core)
    dxp = ((1 - xl) * 4 + z, c)
    pxp = ((1 - xl) * 4 + z, y * 4 + (1 - xh) * 2 + core)
    xo = (r, y * 4 + (1 - xh) * 2 + core)
    yu, yo, yd = ((r, ((y + k) % 4) * 4 + low) for k in (1, 2, 3))
    zu, zo, zd = ((xl * 4 + (z + k) % 4, c) for k in (1, 2, 3))

    count = [0]
    pending = []

    def send(src, dst, device):
        k = count[0]
        count[0] += 1
        copy = pltpu.make_async_remote_copy(
            src_ref=src, dst_ref=dst, send_sem=send_sem.at[k], recv_sem=recv_sem.at[k],
            device_id=device, device_id_type=MESH,
        )
        copy.start()
        pending.append(copy)
        return copy

    loads = [
        pltpu.make_async_copy(src, dst, in_sem.at[k])
        for k, (src, dst) in enumerate(zip(hbm, (x_ref, p_ref, region_ref, match_ref)))
    ]
    for load in loads:
        load.start()
    barrier = pltpu.get_barrier_semaphore()
    for peer in (cp, dxp, pxp, xo, yu, yo, yd, zu, zo, zd):
        pl.semaphore_signal(barrier, inc=1, device_id=peer, device_id_type=MESH)
    own_x, own_p = xs(0, 0), ps(0, 0)
    acc[...] = jnp.zeros_like(acc)
    for load in loads:
        load.wait()
    xb[rows(own_x), :] = normalize(x_ref)[0].astype(bf16)
    pb[rows(own_p), :] = normalize(p_ref)[0].astype(bf16)
    xo_ref[...] = x_ref[...]
    po_ref[...] = p_ref[...]
    packed = match_ref[...] * 64 + region_ref[...]
    wide = jnp.concatenate([packed, jnp.zeros((1, 64), i32)], axis=1)
    lab_ref[0] = jnp.concatenate([wide, pltpu.roll(wide, 64, 1)], axis=1)
    lx[own_x] = wide
    lp[own_p] = lab_ref[0]
    pl.semaphore_wait(barrier, 10)

    got = {}

    def send_x(src, dst, device, h):
        if h == 0:
            label = lab_ref.at[0, :, pl.ds(0, 256)] if src == own_x else lx.at[src]
            got["x", dst, "label"] = send(label, lx.at[dst], device)
        got["x", dst, h] = send(xb.at[part(src, h)], xb.at[part(dst, h)], device)

    def send_p(src, dst, device, h):
        if h == 0:
            label = lab_ref.at[0] if src == own_p else lp.at[src]
            got["p", dst, "label"] = send(label, lp.at[dst], device)
        got["p", dst, h] = send(pb.at[part(src, h)], pb.at[part(dst, h)], device)

    def wait(kind, slot, h):
        if h == 0:
            got[kind, slot, "label"].wait_recv()
        got[kind, slot, h].wait_recv()

    def send_core(u):
        src, dst = xs(*u), xs(*u, 1)
        label = lab_ref.at[0, :, pl.ds(0, 256)] if src == own_x else lx.at[src]
        got["core", u] = (send(label, lx.at[dst], cp), send(xb.at[rows(src)], xb.at[rows(dst)], cp))

    def row_info(slot):
        t = jnp.transpose(jnp.broadcast_to(lx[slot], (128, 256)))[0:B]
        rr[rows(slot), :] = t & 63
        rm[rows(slot), :] = t >> 6

    def rows_ready(u):
        row_info(xs(*u))
        for copy in got["core", u]:
            copy.wait_recv()
        row_info(xs(*u, 1))

    def base(rz_, rx):
        zz = (z + rz_) % 4
        if rx == 0:
            return ((xl * 4 + zz) * 16 + y * 4 + xh * 2 + core) * B
        return (((1 - xl) * 4 + zz) * 16 + y * 4 + (1 - xh) * 2 + core) * B

    def col_info(k0):
        first, second = lp[k0], lp[k0 + 1]
        base0, base1 = base(*PU[k0]), base(*PU[k0 + 1])
        lane = lax.broadcasted_iota(i32, (1, 128), 1)
        parts = (first[:, 0:128], first[:, 128:256] + second[:, 256:384], second[:, 384:512])
        for k in range(3):
            at = lane + k * 128
            cs = pl.ds(k0 * B + k * 128, 128)
            cr[:, cs] = parts[k] & 63
            cj[:, cs] = jnp.where(at < B, base0 + at, base1 + at - B)

    for h in (0, 1):
        send_x(own_x, xs(0, 1), dxp, h)
        send_p(own_p, ps(0, 1), pxp, h)
        send_x(own_x, xs(3, 0), yu, h)
        send_x(own_x, xs(1, 0), yd, h)
        send_p(own_p, ps(3, 0), zu, h)
        send_p(own_p, ps(1, 0), zd, h)
    send_core((0, 0))

    gain = gain_ref[...] / E
    gain2 = gain * LOG2E
    shift2 = shift_ref[...] * LOG2E

    def tile(v, c0, width, new_row=False, new_col=False, add_col=None):
        r0 = v * V
        x = xb[pl.ds(r0, V), :]
        p = pb[pl.ds(c0, width), :]
        s = lax.dot_general(x, p, NT, preferred_element_type=f32)
        region, match = rr[pl.ds(r0, V), :], rm[pl.ds(r0, V), :]
        slopes, total = [], None
        for k in range(width // 128):
            cs = pl.ds(c0 + k * 128, 128)
            slope, soft = pair_terms(
                s[:, k * 128 : (k + 1) * 128], region, match, cr[:, cs], cj[:, cs], gain, gain2, shift2
            )
            slopes.append(slope)
            soft = fold(soft)
            total = soft if total is None else total + soft
        acc[...] += total
        g = jnp.concatenate(slopes, axis=1)
        d_row = lax.dot_general(g, p, NN, preferred_element_type=f32)
        dx[pl.ds(r0, V), :] = d_row if new_row else dx[pl.ds(r0, V), :] + d_row
        cut = width if new_col else 0 if add_col is None else add_col - c0
        for lo, hi, new in ((0, cut, True), (cut, width, False)):
            if lo < hi:
                d_col = lax.dot_general(g[:, lo:hi], x, TN, preferred_element_type=f32)
                at = pl.ds(c0 + lo, hi - lo)
                dp[at, :] = d_col if new else dp[at, :] + d_col

    C1, END = 512, 2 * V

    def cols(v, lo, hi, **new):
        tile(v, lo, hi - lo, **new)

    for h in (0, 1):
        wait("x", xs(3, 0), h)
        send_x(xs(3, 0), xs(2, 0), yu, h)
        wait("p", ps(3, 0), h)
        send_p(ps(3, 0), ps(2, 0), zu, h)
        wait("x", xs(0, 1), h)
        send_x(xs(0, 1), xs(1, 1), yd, h)
        wait("p", ps(0, 1), h)
        send_p(ps(0, 1), ps(1, 1), zd, h)
    for h in (0, 1):
        send_x(xs(0, 1), xs(3, 1), yu, h)
        send_p(ps(0, 1), ps(3, 1), zu, h)
    send_core((0, 1))
    send_core((3, 0))
    for h in (0, 1):
        wait("x", xs(1, 0), h)
    send_core((1, 0))
    for h in (0, 1):
        wait("p", ps(1, 0), h)
    col_info(4)
    col_info(6)
    rows_ready((0, 0))
    rows_ready((0, 1))
    cols(0, V, V + 384, new_row=True, new_col=True)
    for h in (0, 1):
        wait("x", xs(1, 1), h)
        send_x(xs(1, 1), xs(2, 1), yd, h)
        wait("p", ps(1, 1), h)
        send_p(ps(1, 1), ps(2, 1), zd, h)
        if h == 0:
            cols(0, V + 384, END, new_col=True)
    send_core((1, 1))
    for h in (0, 1):
        wait("x", xs(2, 0), h)
    send_core((2, 0))
    rows_ready((3, 0))
    rows_ready((1, 0))
    cols(1, V, END, new_row=True)
    rows_ready((2, 0))
    rows_ready((1, 1))

    for h in (0, 1):
        wait("x", xs(2, 1), h)
    send_core((2, 1))
    for h in (0, 1):
        wait("x", xs(3, 1), h)
    send_core((3, 1))
    row_info(xs(3, 1))
    for u in ((2, 0), (2, 1), (3, 1)):
        for h in (0, 1):
            wait("p", ps(*u), h)
    col_info(0)
    col_info(2)
    rows_ready((2, 1))
    cols(3, 0, END, new_row=True, add_col=V)

    half = {}
    back = {}

    def to_core(u):
        half[u] = send(dx.at[rows(xs(*u, 1))], rc.at[XU.index(u)], cp)

    def add_core(u):
        half[u].wait_recv()
        dx[rows(xs(*u)), :] += rc[XU.index(u)]

    def cut(slot, h, first):
        return pl.ds(slot * B + h * first, B - first if h else first)

    def send_dx(u, k, device, h):
        back["x", k, h] = send(dx.at[cut(xs(*u), h, CUT_X)], ry.at[k, cut(0, h, CUT_X)], device)

    def send_dp(u, k, device, h):
        back["p", k, h] = send(dp.at[cut(ps(*u), h, CUT_P)], rz.at[k, cut(0, h, CUT_P)], device)

    def add_dx(u, k, h):
        back["x", k, h].wait_recv()
        dx[cut(xs(*u), h, CUT_X), :] += ry[k, cut(0, h, CUT_X)]

    def add_dp(u, k, h):
        back["p", k, h].wait_recv()
        dp[cut(ps(*u), h, CUT_P), :] += rz[k, cut(0, h, CUT_P)]

    ring = {}

    def loss_send(k, peers):
        for n, peer in enumerate(peers):
            ring[k, n] = send(lsend.at[k], lrecv.at[3 * k + n], peer)

    def loss_add(k, n):
        for m in range(n):
            ring[k, m].wait_recv()
        if n == 1:
            lsend[k + 1] = lsend[k] + lrecv[3 * k]
        else:
            lsend[k + 1] = (lsend[k] + lrecv[3 * k]) + (lrecv[3 * k + 1] + lrecv[3 * k + 2])

    to_core((2, 0))
    to_core((2, 1))
    cols(0, 0, C1)
    add_core((2, 0))
    add_core((2, 1))
    for h in (0, 1):
        send_dx((2, 0), 0, yd, h)
        send_dx((2, 1), 1, yu, h)
    cols(1, 0, C1)
    for copy in got["core", (3, 1)]:
        copy.wait_recv()
    row_info(xs(3, 1, 1))
    cols(2, 0, C1, new_row=True)
    for h in (0, 1):
        send_dp((2, 0), 0, zd, h)
        send_dp((2, 1), 1, zu, h)
    cols(2, C1, END)
    to_core((1, 1))
    to_core((3, 1))
    send_dp((0, 1), 6, pxp, 1)
    cols(0, C1, V)
    add_core((1, 1))
    add_core((3, 1))
    send_dx((3, 1), 3, dxp, 1)
    send_dx((3, 1), 3, yd, 0)
    add_dx((1, 1), 1, 0)
    send_dx((1, 1), 5, yu, 0)
    cols(1, C1, V)
    lsend[0] = jnp.sum(acc[...], axis=0, keepdims=True)
    loss_send(0, (cp,))
    for u in ((3, 0), (1, 0), (0, 1), (0, 0)):
        to_core(u)
    add_dx((1, 1), 1, 1)
    send_dx((1, 1), 5, dxp, 1)
    send_dp((3, 1), 3, pxp, 1)
    loss_add(0, 1)
    loss_send(1, (zo, zu, zd))
    send_dp((3, 1), 3, zd, 0)
    add_dp((1, 1), 1, 0)
    send_dp((1, 1), 5, zu, 0)
    add_dp((3, 0), 0, 0)
    send_dp((3, 0), 2, zd, 0)
    send_dp((1, 0), 4, zu, 0)
    add_core((3, 0))
    add_dx((3, 0), 0, 0)
    add_core((1, 0))
    add_core((0, 1))
    add_core((0, 0))
    add_dx((3, 0), 0, 1)
    add_dp((1, 1), 1, 1)
    send_dp((1, 1), 5, pxp, 1)
    add_dp((3, 0), 0, 1)
    loss_add(1, 3)
    loss_send(2, (yo, yu, yd))
    send_dx((3, 0), 2, yd, 0)
    send_dx((1, 0), 4, yu, 0)
    add_dx((0, 1), 3, 0)
    add_dx((0, 1), 5, 0)
    send_dx((0, 1), 6, dxp, 0)
    add_dx((3, 0), 3, 1)
    send_dx((3, 0), 2, yd, 1)
    add_dp((3, 0), 3, 1)
    send_dp((3, 0), 2, zd, 1)
    loss_add(2, 3)
    loss_send(3, (xo, dxp, pxp))
    send_dx((0, 1), 6, dxp, 1)
    add_dx((1, 0), 5, 1)
    send_dx((1, 0), 4, yu, 1)
    add_dp((0, 1), 3, 0)
    add_dp((0, 1), 5, 0)
    send_dp((0, 1), 6, pxp, 0)
    add_dp((1, 0), 5, 1)
    send_dp((1, 0), 4, zu, 1)
    add_dx((0, 0), 2, 0)
    add_dx((0, 0), 4, 0)
    add_dp((0, 0), 6, 1)
    loss_add(3, 3)
    loss_ref[...] = lsend[4]
    add_dx((0, 0), 6, 0)
    add_dp((0, 0), 2, 0)
    add_dp((0, 0), 4, 0)
    add_dx((0, 0), 4, 1)
    add_dx((0, 0), 2, 1)
    add_dx((0, 0), 6, 1)
    sx_ref[...] = dx[rows(own_x), :]
    add_dp((0, 0), 4, 1)
    add_dp((0, 0), 2, 1)
    add_dp((0, 0), 6, 0)
    sp_ref[...] = dp[rows(own_p), :]
    for copy in pending:
        copy.wait_send()
    assert count[0] == N_SEM


def finish(x_ref, p_ref, sx_ref, sp_ref, sum_ref, loss_ref, gx_ref, gp_ref):
    for ref, sums, out in ((x_ref, sx_ref, gx_ref), (p_ref, sp_ref, gp_ref)):
        full, scale = normalize(ref)
        dnorm = sums[...]
        out[...] = scale * (dnorm - full * jnp.mean(dnorm * full, axis=-1, keepdims=True))
    n = float(128 * B)
    loss_ref[0] = jnp.sum(sum_ref[...]) * LN2 / (n * n)


def on_device(lensed, theta, region, match, gain, shift):
    vmem = pl.BlockSpec(memory_space=pltpu.VMEM)
    lensed, theta, region, match = (
        pltpu.with_memory_space_constraint(a, pltpu.HBM) for a in (lensed, theta, region.reshape(1, B), match.reshape(1, B))
    )
    smem = pl.BlockSpec(memory_space=pltpu.SMEM)
    block = jax.ShapeDtypeStruct((B, E), f32)
    half = jax.ShapeDtypeStruct((B, E), bf16)
    total, sum_x, sum_p, x, p = pl.pallas_call(
        kernel,
        out_shape=(jax.ShapeDtypeStruct((1, 128), f32), block, block, half, half),
        in_specs=[vmem] * 2 + [pl.BlockSpec(memory_space=pltpu.HBM)] * 4,
        out_specs=(vmem,) * 5,
        scratch_shapes=[
            pltpu.VMEM((B, E), bf16),
            pltpu.VMEM((B, E), bf16),
            pltpu.VMEM((1, B), i32),
            pltpu.VMEM((1, B), i32),
            pltpu.SemaphoreType.DMA((4,)),
            pltpu.VMEM((16 * B, E), bf16),
            pltpu.VMEM((8 * B, E), bf16),
            pltpu.VMEM((1, 1, 512), i32),
            pltpu.VMEM((16, 1, 256), i32),
            pltpu.VMEM((8, 1, 512), i32),
            pltpu.VMEM((16 * B, 128), i32),
            pltpu.VMEM((16 * B, 128), i32),
            pltpu.VMEM((1, 8 * B), i32),
            pltpu.VMEM((1, 8 * B), i32),
            pltpu.VMEM((16 * B, E), f32),
            pltpu.VMEM((8 * B, E), f32),
            pltpu.VMEM((8, B, E), f32),
            pltpu.VMEM((7, B, E), f32),
            pltpu.VMEM((7, B, E), f32),
            pltpu.VMEM((8, 128), f32),
            pltpu.VMEM((5, 1, 128), f32),
            pltpu.VMEM((12, 1, 128), f32),
            pltpu.SemaphoreType.DMA((N_SEM,)),
            pltpu.SemaphoreType.DMA((N_SEM,)),
        ],
        compiler_params=pltpu.CompilerParams(
            collective_id=0, has_side_effects=True, vmem_limit_bytes=48 << 20
        ),
        name="pairs",
    )(gain.reshape(1, 1), shift.reshape(1, 1), lensed, theta, region, match)
    return pl.pallas_call(
        finish,
        out_shape=(jax.ShapeDtypeStruct((1,), f32), block, block),
        in_specs=[vmem] * 5,
        out_specs=(smem, vmem, vmem),
        compiler_params=pltpu.CompilerParams(vmem_limit_bytes=8 << 20),
        name="finish",
    )(x, p, sum_x, sum_p, total)


def solution(mesh):
    both = ("row", "col")
    in_specs = (P(both, None), P(both, None), P(both), P(both), P(), P())
    out_specs = (P(), P(both, None), P(both, None))
    return jax.shard_map(
        on_device, mesh=mesh, in_specs=in_specs, out_specs=out_specs, check_vma=False
    )
```

```python
import jax
import jax.numpy as jnp
from jax import lax
from jax.experimental import pallas as pl
from jax.experimental.pallas import tpu as pltpu
from jax.sharding import PartitionSpec as P

f32 = jnp.float32
bf16 = jnp.bfloat16
i32 = jnp.int32
LOG2E = 1.4426950408889634
LN2 = 0.6931471805599453
MASKED = -1e5
NT = (((1,), (1,)), ((), ()))
NN = (((1,), (0,)), ((), ()))
TN = (((0,), (0,)), ((), ()))
MESH = pl.DeviceIdType.MESH
B = 192
E = 512
V = 4 * B
H = B // 2
CUT_X, CUT_P = 120, 112
XU = [(0, 0), (0, 1), (3, 0), (1, 0), (3, 1), (1, 1), (2, 0), (2, 1)]
PU = [(2, 0), (2, 1), (3, 1), (1, 1), (0, 0), (0, 1), (3, 0), (1, 0)]
N_SEM = 7 * 3 + 8 * 2 + 7 * 3 + 8 + 2 * 7 * 2 + 10


def xs(ry, rx, rc=0):
    return 2 * XU.index((ry, rx)) + rc


def ps(rz, rx):
    return PU.index((rz, rx))


def part(slot, h):
    return pl.ds(slot * B + h * H, H)


def rows(slot):
    return pl.ds(slot * B, B)


def pair_terms(s, row_region, row_match, col_region, col_index, gain, gain2, shift2):
    t = s * gain2 + shift2
    positive = row_match == col_index
    t = jnp.where(positive, -t, jnp.where(row_region != col_region, t, MASKED))
    soft = jnp.log2(1.0 + jnp.exp2(t))
    slope = jnp.exp2(t - soft) * jnp.where(positive, -gain, gain)
    return slope.astype(bf16), soft


def fold(x):
    return jnp.sum(x.reshape(x.shape[0] // 8, 8, 128), axis=0)


def normalize(ref):
    full = ref[...].astype(f32)
    scale = lax.rsqrt(jnp.mean(full * full, axis=-1, keepdims=True) + 1e-06)
    return full * scale, scale


def kernel(
    gain_ref, shift_ref, *hbm_and_rest,
):
    hbm, rest = hbm_and_rest[:4], hbm_and_rest[4:]
    pair_kernel(gain_ref, shift_ref, hbm, *rest)


def pair_kernel(
    gain_ref, shift_ref, hbm,
    loss_ref, sx_ref, sp_ref, xo_ref, po_ref,
    x_ref, p_ref, region_ref, match_ref, in_sem,
    xb, pb, lab_ref, lx, lp, rr, rm, cr, cj, dx, dp, rc, ry, rz, acc, lsend, lrecv, send_sem, recv_sem,
):
    r, c = lax.axis_index("row"), lax.axis_index("col")
    xl, z = r // 4, r % 4
    y, xh, core = c // 4, (c // 2) % 2, c % 2
    low = c % 4
    cp = (r, c + 1 - 2 * core)
    dxp = ((1 - xl) * 4 + z, c)
    pxp = ((1 - xl) * 4 + z, y * 4 + (1 - xh) * 2 + core)
    xo = (r, y * 4 + (1 - xh) * 2 + core)
    yu, yo, yd = ((r, ((y + k) % 4) * 4 + low) for k in (1, 2, 3))
    zu, zo, zd = ((xl * 4 + (z + k) % 4, c) for k in (1, 2, 3))

    count = [0]
    pending = []

    def send(src, dst, device):
        k = count[0]
        count[0] += 1
        copy = pltpu.make_async_remote_copy(
            src_ref=src, dst_ref=dst, send_sem=send_sem.at[k], recv_sem=recv_sem.at[k],
            device_id=device, device_id_type=MESH,
        )
        copy.start()
        pending.append(copy)
        return copy

    loads = [
        pltpu.make_async_copy(src, dst, in_sem.at[k])
        for k, (src, dst) in enumerate(zip(hbm, (x_ref, p_ref, region_ref, match_ref)))
    ]
    for load in loads:
        load.start()
    barrier = pltpu.get_barrier_semaphore()
    for peer in (cp, dxp, pxp, xo, yu, yo, yd, zu, zo, zd):
        pl.semaphore_signal(barrier, inc=1, device_id=peer, device_id_type=MESH)
    own_x, own_p = xs(0, 0), ps(0, 0)
    acc[...] = jnp.zeros_like(acc)
    for load in loads:
        load.wait()
    xb[rows(own_x), :] = normalize(x_ref)[0].astype(bf16)
    pb[rows(own_p), :] = normalize(p_ref)[0].astype(bf16)
    xo_ref[...] = x_ref[...]
    po_ref[...] = p_ref[...]
    packed = match_ref[...] * 64 + region_ref[...]
    wide = jnp.concatenate([packed, jnp.zeros((1, 64), i32)], axis=1)
    lab_ref[0] = jnp.concatenate([wide, pltpu.roll(wide, 64, 1)], axis=1)
    lx[own_x] = wide
    lp[own_p] = lab_ref[0]
    pl.semaphore_wait(barrier, 10)

    got = {}

    def send_x(src, dst, device, h):
        if h == 0:
            label = lab_ref.at[0, :, pl.ds(0, 256)] if src == own_x else lx.at[src]
            got["x", dst, "label"] = send(label, lx.at[dst], device)
        got["x", dst, h] = send(xb.at[part(src, h)], xb.at[part(dst, h)], device)

    def send_p(src, dst, device, h):
        if h == 0:
            label = lab_ref.at[0] if src == own_p else lp.at[src]
            got["p", dst, "label"] = send(label, lp.at[dst], device)
        got["p", dst, h] = send(pb.at[part(src, h)], pb.at[part(dst, h)], device)

    def wait(kind, slot, h):
        if h == 0:
            got[kind, slot, "label"].wait_recv()
        got[kind, slot, h].wait_recv()

    def send_core(u):
        src, dst = xs(*u), xs(*u, 1)
        label = lab_ref.at[0, :, pl.ds(0, 256)] if src == own_x else lx.at[src]
        got["core", u] = (send(label, lx.at[dst], cp), send(xb.at[rows(src)], xb.at[rows(dst)], cp))

    def row_info(slot):
        t = jnp.transpose(jnp.broadcast_to(lx[slot], (128, 256)))[0:B]
        rr[rows(slot), :] = t & 63
        rm[rows(slot), :] = t >> 6

    def rows_ready(u):
        row_info(xs(*u))
        for copy in got["core", u]:
            copy.wait_recv()
        row_info(xs(*u, 1))

    def base(rz_, rx):
        zz = (z + rz_) % 4
        if rx == 0:
            return ((xl * 4 + zz) * 16 + y * 4 + xh * 2 + core) * B
        return (((1 - xl) * 4 + zz) * 16 + y * 4 + (1 - xh) * 2 + core) * B

    def col_info(k0):
        first, second = lp[k0], lp[k0 + 1]
        base0, base1 = base(*PU[k0]), base(*PU[k0 + 1])
        lane = lax.broadcasted_iota(i32, (1, 128), 1)
        parts = (first[:, 0:128], first[:, 128:256] + second[:, 256:384], second[:, 384:512])
        for k in range(3):
            at = lane + k * 128
            cs = pl.ds(k0 * B + k * 128, 128)
            cr[:, cs] = parts[k] & 63
            cj[:, cs] = jnp.where(at < B, base0 + at, base1 + at - B)

    for h in (0, 1):
        send_x(own_x, xs(0, 1), dxp, h)
        send_p(own_p, ps(0, 1), pxp, h)
        send_x(own_x, xs(3, 0), yu, h)
        send_x(own_x, xs(1, 0), yd, h)
        send_p(own_p, ps(3, 0), zu, h)
        send_p(own_p, ps(1, 0), zd, h)
    send_core((0, 0))

    gain = gain_ref[...] / E
    gain2 = gain * LOG2E
    shift2 = shift_ref[...] * LOG2E

    def tile(v, c0, width, new_row=False, new_col=False, add_col=None):
        r0 = v * V
        x = xb[pl.ds(r0, V), :]
        p = pb[pl.ds(c0, width), :]
        s = lax.dot_general(x, p, NT, preferred_element_type=f32)
        region, match = rr[pl.ds(r0, V), :], rm[pl.ds(r0, V), :]
        slopes, total = [], None
        for k in range(width // 128):
            cs = pl.ds(c0 + k * 128, 128)
            slope, soft = pair_terms(
                s[:, k * 128 : (k + 1) * 128], region, match, cr[:, cs], cj[:, cs], gain, gain2, shift2
            )
            slopes.append(slope)
            soft = fold(soft)
            total = soft if total is None else total + soft
        acc[...] += total
        g = jnp.concatenate(slopes, axis=1)
        d_row = lax.dot_general(g, p, NN, preferred_element_type=f32)
        dx[pl.ds(r0, V), :] = d_row if new_row else dx[pl.ds(r0, V), :] + d_row
        cut = width if new_col else 0 if add_col is None else add_col - c0
        for lo, hi, new in ((0, cut, True), (cut, width, False)):
            if lo < hi:
                d_col = lax.dot_general(g[:, lo:hi], x, TN, preferred_element_type=f32)
                at = pl.ds(c0 + lo, hi - lo)
                dp[at, :] = d_col if new else dp[at, :] + d_col

    C1, END = 512, 2 * V

    def cols(v, lo, hi, **new):
        tile(v, lo, hi - lo, **new)

    for h in (0, 1):
        wait("x", xs(3, 0), h)
        send_x(xs(3, 0), xs(2, 0), yu, h)
        wait("p", ps(3, 0), h)
        send_p(ps(3, 0), ps(2, 0), zu, h)
        wait("x", xs(0, 1), h)
        send_x(xs(0, 1), xs(1, 1), yd, h)
        wait("p", ps(0, 1), h)
        send_p(ps(0, 1), ps(1, 1), zd, h)
    for h in (0, 1):
        send_x(xs(0, 1), xs(3, 1), yu, h)
        send_p(ps(0, 1), ps(3, 1), zu, h)
    send_core((0, 1))
    send_core((3, 0))
    for h in (0, 1):
        wait("x", xs(1, 0), h)
    send_core((1, 0))
    for h in (0, 1):
        wait("p", ps(1, 0), h)
    col_info(4)
    col_info(6)
    rows_ready((0, 0))
    rows_ready((0, 1))
    cols(0, V, V + 384, new_row=True, new_col=True)
    for h in (0, 1):
        wait("x", xs(1, 1), h)
        send_x(xs(1, 1), xs(2, 1), yd, h)
        wait("p", ps(1, 1), h)
        send_p(ps(1, 1), ps(2, 1), zd, h)
        if h == 0:
            cols(0, V + 384, END, new_col=True)
    send_core((1, 1))
    for h in (0, 1):
        wait("x", xs(2, 0), h)
    send_core((2, 0))
    rows_ready((3, 0))
    rows_ready((1, 0))
    cols(1, V, END, new_row=True)
    rows_ready((2, 0))
    rows_ready((1, 1))

    for h in (0, 1):
        wait("x", xs(2, 1), h)
    send_core((2, 1))
    for h in (0, 1):
        wait("x", xs(3, 1), h)
    send_core((3, 1))
    row_info(xs(3, 1))
    for u in ((2, 0), (2, 1), (3, 1)):
        for h in (0, 1):
            wait("p", ps(*u), h)
    col_info(0)
    col_info(2)
    rows_ready((2, 1))
    cols(3, 0, END, new_row=True, add_col=V)

    half = {}
    back = {}

    def to_core(u):
        half[u] = send(dx.at[rows(xs(*u, 1))], rc.at[XU.index(u)], cp)

    def add_core(u):
        half[u].wait_recv()
        dx[rows(xs(*u)), :] += rc[XU.index(u)]

    def cut(slot, h, first):
        return pl.ds(slot * B + h * first, B - first if h else first)

    def send_dx(u, k, device, h):
        back["x", k, h] = send(dx.at[cut(xs(*u), h, CUT_X)], ry.at[k, cut(0, h, CUT_X)], device)

    def send_dp(u, k, device, h):
        back["p", k, h] = send(dp.at[cut(ps(*u), h, CUT_P)], rz.at[k, cut(0, h, CUT_P)], device)

    def add_dx(u, k, h):
        back["x", k, h].wait_recv()
        dx[cut(xs(*u), h, CUT_X), :] += ry[k, cut(0, h, CUT_X)]

    def add_dp(u, k, h):
        back["p", k, h].wait_recv()
        dp[cut(ps(*u), h, CUT_P), :] += rz[k, cut(0, h, CUT_P)]

    ring = {}

    def loss_send(k, peers):
        for n, peer in enumerate(peers):
            ring[k, n] = send(lsend.at[k], lrecv.at[3 * k + n], peer)

    def loss_add(k, n):
        for m in range(n):
            ring[k, m].wait_recv()
        if n == 1:
            lsend[k + 1] = lsend[k] + lrecv[3 * k]
        else:
            lsend[k + 1] = (lsend[k] + lrecv[3 * k]) + (lrecv[3 * k + 1] + lrecv[3 * k + 2])

    to_core((2, 0))
    to_core((2, 1))
    cols(0, 0, C1)
    add_core((2, 0))
    add_core((2, 1))
    for h in (0, 1):
        send_dx((2, 0), 0, yd, h)
        send_dx((2, 1), 1, yu, h)
    cols(1, 0, C1)
    for copy in got["core", (3, 1)]:
        copy.wait_recv()
    row_info(xs(3, 1, 1))
    cols(2, 0, C1, new_row=True)
    for h in (0, 1):
        send_dp((2, 0), 0, zd, h)
        send_dp((2, 1), 1, zu, h)
    cols(2, C1, END)
    to_core((1, 1))
    to_core((3, 1))
    send_dp((0, 1), 6, pxp, 1)
    cols(0, C1, V)
    add_core((1, 1))
    add_core((3, 1))
    send_dx((3, 1), 3, dxp, 1)
    send_dx((3, 1), 3, yd, 0)
    add_dx((1, 1), 1, 0)
    send_dx((1, 1), 5, yu, 0)
    cols(1, C1, V)
    lsend[0] = jnp.sum(acc[...], axis=0, keepdims=True)
    loss_send(0, (cp,))
    for u in ((3, 0), (1, 0), (0, 1), (0, 0)):
        to_core(u)
    add_dx((1, 1), 1, 1)
    send_dx((1, 1), 5, dxp, 1)
    send_dp((3, 1), 3, pxp, 1)
    loss_add(0, 1)
    loss_send(1, (zo, zu, zd))
    send_dp((3, 1), 3, zd, 0)
    add_dp((1, 1), 1, 0)
    send_dp((1, 1), 5, zu, 0)
    add_dp((3, 0), 0, 0)
    send_dp((3, 0), 2, zd, 0)
    send_dp((1, 0), 4, zu, 0)
    add_core((3, 0))
    add_dx((3, 0), 0, 0)
    add_core((1, 0))
    add_core((0, 1))
    add_core((0, 0))
    add_dx((3, 0), 0, 1)
    add_dp((1, 1), 1, 1)
    send_dp((1, 1), 5, pxp, 1)
    add_dp((3, 0), 0, 1)
    loss_add(1, 3)
    loss_send(2, (yo, yu, yd))
    send_dx((3, 0), 2, yd, 0)
    send_dx((1, 0), 4, yu, 0)
    add_dx((0, 1), 3, 0)
    add_dx((0, 1), 5, 0)
    send_dx((0, 1), 6, dxp, 0)
    add_dx((3, 0), 3, 1)
    send_dx((3, 0), 2, yd, 1)
    add_dp((3, 0), 3, 1)
    send_dp((3, 0), 2, zd, 1)
    loss_add(2, 3)
    loss_send(3, (xo, dxp, pxp))
    send_dx((0, 1), 6, dxp, 1)
    add_dx((1, 0), 5, 1)
    send_dx((1, 0), 4, yu, 1)
    add_dp((0, 1), 3, 0)
    add_dp((0, 1), 5, 0)
    send_dp((0, 1), 6, pxp, 0)
    add_dp((1, 0), 5, 1)
    send_dp((1, 0), 4, zu, 1)
    add_dx((0, 0), 2, 0)
    add_dx((0, 0), 4, 0)
    add_dp((0, 0), 6, 1)
    loss_add(3, 3)
    loss_ref[...] = lsend[4]
    add_dx((0, 0), 6, 0)
    add_dp((0, 0), 2, 0)
    add_dp((0, 0), 4, 0)
    add_dx((0, 0), 4, 1)
    add_dx((0, 0), 2, 1)
    add_dx((0, 0), 6, 1)
    sx_ref[...] = dx[rows(own_x), :]
    add_dp((0, 0), 4, 1)
    add_dp((0, 0), 2, 1)
    add_dp((0, 0), 6, 0)
    sp_ref[...] = dp[rows(own_p), :]
    for copy in pending:
        copy.wait_send()
    assert count[0] == N_SEM


def finish(x_ref, p_ref, sx_ref, sp_ref, sum_ref, loss_ref, gx_ref, gp_ref):
    for ref, sums, out in ((x_ref, sx_ref, gx_ref), (p_ref, sp_ref, gp_ref)):
        full, scale = normalize(ref)
        dnorm = sums[...]
        out[...] = scale * (dnorm - full * jnp.mean(dnorm * full, axis=-1, keepdims=True))
    n = float(128 * B)
    loss_ref[0] = jnp.sum(sum_ref[...]) * LN2 / (n * n)


def on_device(lensed, theta, region, match, gain, shift):
    vmem = pl.BlockSpec(memory_space=pltpu.VMEM)
    lensed, theta, region, match = (
        pltpu.with_memory_space_constraint(a, pltpu.HBM) for a in (lensed, theta, region.reshape(1, B), match.reshape(1, B))
    )
    smem = pl.BlockSpec(memory_space=pltpu.SMEM)
    block = jax.ShapeDtypeStruct((B, E), f32)
    half = jax.ShapeDtypeStruct((B, E), bf16)
    total, sum_x, sum_p, x, p = pl.pallas_call(
        kernel,
        out_shape=(jax.ShapeDtypeStruct((1, 128), f32), block, block, half, half),
        in_specs=[vmem] * 2 + [pl.BlockSpec(memory_space=pltpu.HBM)] * 4,
        out_specs=(vmem,) * 5,
        scratch_shapes=[
            pltpu.VMEM((B, E), bf16),
            pltpu.VMEM((B, E), bf16),
            pltpu.VMEM((1, B), i32),
            pltpu.VMEM((1, B), i32),
            pltpu.SemaphoreType.DMA((4,)),
            pltpu.VMEM((16 * B, E), bf16),
            pltpu.VMEM((8 * B, E), bf16),
            pltpu.VMEM((1, 1, 512), i32),
            pltpu.VMEM((16, 1, 256), i32),
            pltpu.VMEM((8, 1, 512), i32),
            pltpu.VMEM((16 * B, 128), i32),
            pltpu.VMEM((16 * B, 128), i32),
            pltpu.VMEM((1, 8 * B), i32),
            pltpu.VMEM((1, 8 * B), i32),
            pltpu.VMEM((16 * B, E), f32),
            pltpu.VMEM((8 * B, E), f32),
            pltpu.VMEM((8, B, E), f32),
            pltpu.VMEM((7, B, E), f32),
            pltpu.VMEM((7, B, E), f32),
            pltpu.VMEM((8, 128), f32),
            pltpu.VMEM((5, 1, 128), f32),
            pltpu.VMEM((12, 1, 128), f32),
            pltpu.SemaphoreType.DMA((N_SEM,)),
            pltpu.SemaphoreType.DMA((N_SEM,)),
        ],
        compiler_params=pltpu.CompilerParams(
            collective_id=0, has_side_effects=True, vmem_limit_bytes=48 << 20
        ),
        name="pairs",
    )(gain.reshape(1, 1), shift.reshape(1, 1), lensed, theta, region, match)
    return pl.pallas_call(
        finish,
        out_shape=(jax.ShapeDtypeStruct((1,), f32), block, block),
        in_specs=[vmem] * 5,
        out_specs=(smem, vmem, vmem),
        compiler_params=pltpu.CompilerParams(vmem_limit_bytes=8 << 20),
        name="finish",
    )(x, p, sum_x, sum_p, total)


def solution(mesh):
    both = ("row", "col")
    in_specs = (P(both, None), P(both, None), P(both), P(both), P(), P())
    out_specs = (P(), P(both, None), P(both, None))
    return jax.shard_map(
        on_device, mesh=mesh, in_specs=in_specs, out_specs=out_specs, check_vma=False
    )
```
